128 devices in a mesh: tm: 32 (over y, x, core), space: 4 (over z).
Axes of the slice: x: 4, y: 4, z: 4, core: 2. Of those that a mesh axis runs over, the one named last changes fastest.
Arguments:
- previous_end: float32 [32, 16, 256, 256], P('tm', 'space'), may hold values from -6 to 6
- source: float32 [32, 16, 256, 256], P('tm', 'space'), may hold values from -4 to 4
- rate: float32 [16, 256, 256], P('space'), may hold values from 0.05 to 0.8
Outputs:
- fine_nodes: float32 [32, 2, 16, 256, 256], P('tm', None, 'space')
The draws below stay inside these ranges and needn't reach their ends.
All inputs are finite; a program needn't handle non-finite values.
Results may differ from the reference program's by a relative error of at most 0.00026.
Values sent between devices are 32-bit elements; how exact they have to be, the bound alone decides.
A program may use at most 128 MiB of HBM per device.

```python
import math
import jax
import jax.numpy as jnp
from jax import lax

NX = 256
NY = 256
TIME = 32
NZ = 16


def levels(key, dims, split, smallest, high):
    factor_of = 1.0
    for axis_at, shards_of in split:
        steps = jax.random.uniform(jax.random.fold_in(jax.random.fold_in(key, 6), axis_at), (shards_of,), jnp.float32, smallest / len(split), high / len(split))
        factor_of = factor_of * jnp.repeat(jnp.exp(steps), dims[axis_at] // shards_of).reshape((-1,) + (1,) * (len(dims) - 1 - axis_at))
    return factor_of


def scatter_about(rng, shape, spread, reach, cuts=(), held_as=jnp.bfloat16):
    drawn = jax.random.normal(rng, shape, jnp.float32) * spread
    if len(cuts) > 0:
        drawn = levels(rng, shape, cuts, -0.22, 0.18) * drawn
    return jnp.clip(drawn, min=-reach, max=reach).astype(held_as)


def setup_inputs(seed: int = 0) -> dict:
    splits = jax.random.split(jax.random.key(seed), 4)
    return {
        "previous_end": scatter_about(splits[0], (TIME, NZ, NX, NY), 1.0, 6.0, ((0, 32), (1, 4)), jnp.float32),
        "source": scatter_about(splits[1], (TIME, NZ, NX, NY), 0.5, 4.0, ((0, 32), (1, 4)), jnp.float32),
        "rate": jnp.clip(jnp.exp(math.log(0.8) - 2.7725887 * jax.random.uniform(splits[2], (NZ, NX, NY), jnp.float32) ** levels(splits[2], (NZ, NX, NY), ((0, 4),), -0.2, 0.2)), 0.05, 0.8),
    }


diffusion = 0.1
speed_z = 0.4
speed_x = 0.3
speed_y = 0.2
weights_one = (5.0 / 24.0, 1.0 / 3.0, -1.0 / 24.0)
weights_two = (-1.0 / 24.0, 1.0 / 3.0, 5.0 / 24.0)


def tendency(padded, rate_field, source_term, spacing):
    middle = padded[..., 1:-1, :, :]
    upper_z = padded[..., 2:, :, :]
    lower_z = padded[..., :-2, :, :]
    plus_x = jnp.roll(middle, -1, axis=-2)
    minus_x = jnp.roll(middle, 1, axis=-2)
    plus_y = jnp.roll(middle, -1, axis=-1)
    minus_y = jnp.roll(middle, 1, axis=-1)
    laplacian = (upper_z + lower_z + plus_x + minus_x + plus_y + minus_y - 6.0 * middle) / (spacing * spacing)
    transport = (speed_z * (upper_z - lower_z) + speed_x * (plus_x - minus_x) + speed_y * (plus_y - minus_y)) / (2.0 * spacing)
    return diffusion * laplacian - transport + rate_field * middle / (1.0 + middle * middle) + source_term


def pad_depth(field, width):
    return jnp.pad(field, [(0, 0)] * (field.ndim - 3) + [(width, width), (0, 0), (0, 0)])


def restrict(field):
    count_z, count_x, count_y = field.shape[-3:]
    blocks = field.reshape(field.shape[:-3] + (count_z // 2, 2, count_x // 2, 2, count_y // 2, 2))
    return jnp.mean(blocks, axis=(-5, -3, -1))


def inject(coarse):
    return jnp.repeat(jnp.repeat(jnp.repeat(coarse, 2, axis=-3), 2, axis=-2), 2, axis=-1)


def reference(previous_end, source, rate):
    restart = previous_end[-1]
    restart_c = restrict(restart)
    rate_c = restrict(rate)
    sources_c = lax.map(restrict, source)

    def turn(start, source_c):
        first = start + 0.5 * tendency(pad_depth(start, 1), rate_c, source_c, 2.0)
        second = first + 0.5 * tendency(pad_depth(first, 1), rate_c, source_c, 2.0)
        return second, (start, first, second)

    last_value, chained = lax.scan(turn, restart_c, sources_c)
    starts, firsts, seconds = chained

    def per_rank(items):
        warm, source_r, start, first, second = items
        warm_c = restrict(warm)
        guess = jnp.stack([restart + inject(start - restart_c), warm + inject(first - warm_c), warm + inject(second - warm_c)])
        images = tendency(pad_depth(guess, 1), rate, source_r, 1.0)
        node_one = guess[0] + (weights_one[0] * images[0] + weights_one[1] * images[1] + weights_one[2] * images[2])
        again = tendency(pad_depth(node_one, 1), rate, source_r, 1.0)
        node_two = node_one + 0.5 * (again - images[1]) + (weights_two[0] * images[0] + weights_two[1] * images[1] + weights_two[2] * images[2])
        return jnp.stack([node_one, node_two])

    return lax.map(per_rank, (previous_end, source, starts, firsts, seconds))
```

```python
import jax
import jax.numpy as jnp
from jax import lax
from jax.experimental import pallas as pl
from jax.experimental.pallas import tpu as pltpu
from jax.sharding import Mesh
from jax.sharding import PartitionSpec as P

TM = ("tm_0", "tm_1", "tm_2")
AXES = TM + ("space",)
MESH = pl.DeviceIdType.MESH
F32 = jnp.float32

diffusion = 0.1
speed_z = 0.4
speed_x = 0.3
speed_y = 0.2
weights_one = (5.0 / 24.0, 1.0 / 3.0, -1.0 / 24.0)
weights_two = (-1.0 / 24.0, 1.0 / 3.0, 5.0 / 24.0)


def stencil_weights(spacing):
    d = diffusion / (spacing * spacing)
    out = [-6.0 * d]
    for speed in (speed_z, speed_x, speed_y):
        out += [d - speed / (2.0 * spacing), d + speed / (2.0 * spacing)]
    return out


def pair_table(fine, coarse):
    rows = lax.broadcasted_iota(jnp.int32, (fine, coarse), 0) // 2
    columns = lax.broadcasted_iota(jnp.int32, (fine, coarse), 1)
    return (rows == columns).astype(F32)


def pooled(total, pair, scratch):
    scratch[...] = jnp.dot(
        total, pair, precision=lax.Precision.HIGHEST, preferred_element_type=F32
    )
    return scratch[pl.ds(0, 128, stride=2), :] + scratch[pl.ds(1, 128, stride=2), :]


def coarse_stage(src, dst, rate, source, row, tiles):
    w = [0.5 * v for v in stencil_weights(2.0)]
    for j in tiles:
        r = 8 + 8 * j
        below = src[0, pl.ds(r, 8), :]
        here = src[1, pl.ds(r, 8), :]
        for k in range(1, 9):
            above = src[k + 1, pl.ds(r, 8), :]
            out = (1.0 + w[0]) * here + source[k - 1, pl.ds(row + 8 * j, 8), :]
            out += w[1] * above + w[2] * below
            out += w[3] * src[k, pl.ds(r + 1, 8), :] + w[4] * src[k, pl.ds(r - 1, 8), :]
            out += w[5] * pltpu.roll(here, 127, 1) + w[6] * pltpu.roll(here, 1, 1)
            out += rate[k - 1, pl.ds(8 * j, 8), :] * here * pl.reciprocal(1.0 + here * here)
            dst[k, pl.ds(r, 8), :] = out
            below, here = here, above


N_SEND = 160


def chain_kernel(
    prev, source, rate,
    states, restart, prev_lo, prev_hi, source_lo, source_hi, rate_lo, rate_hi,
    fine_s, fine_r, fine_p, half, own, buf, rate_c, seed, state_a, state_b,
    edge_out, edge_in, found,
    load_sem, send_sem, slot_sem, seed_sem, rate_sem, edge_sem, state_sem, halo_sem, restart_sem,
):
    y, x, c, z = (lax.axis_index(name) for name in AXES)
    chip = y * 4 + x
    mine = chip * 2 + c
    slab = 2 * z + c
    is_last = mine == 31
    root_chip = chip == 15
    partner = (y, x, 1 - c, z)
    waits = []

    def guarded(cond, action):
        if cond is None:
            action()
        else:
            pl.when(cond)(action)

    def send(src, dst, sem, device, cond=None):
        index = len(waits)

        def build():
            return pltpu.make_async_remote_copy(
                src_ref=src, dst_ref=dst, send_sem=send_sem.at[index], recv_sem=sem,
                device_id=device, device_id_type=MESH,
            )

        waits.append((cond, lambda: build().wait_send()))
        guarded(cond, lambda: build().start())

    def arrived(view, sem, cond=None):
        def wait():
            pltpu.make_async_remote_copy(
                src_ref=view, dst_ref=view, send_sem=send_sem.at[0], recv_sem=sem,
                device_id=partner, device_id_type=MESH,
            ).wait_recv()

        guarded(cond, wait)

    def turned(value):
        return lax.rem(value + 8, 4)

    def first(step):
        return (turned(y + step * c), turned(x + step * (1 - c)), c, z)

    def second(step):
        return (turned(y + step * (1 - c)), turned(x + step * c), c, z)

    def slot(da, db):
        return (turned(y + da * c + db * (1 - c)) * 4 + turned(x + da * (1 - c) + db * c)) * 2 + c

    load_p = pltpu.make_async_copy(prev, fine_p, load_sem.at[0])
    load_s = pltpu.make_async_copy(source, fine_s, load_sem.at[1])
    load_r = pltpu.make_async_copy(rate, fine_r, load_sem.at[2])
    pl.when(is_last)(load_p.start)
    load_s.start()
    load_r.start()
    barrier = pltpu.get_barrier_semaphore()
    peers = [first(1), first(-1), second(1), second(-1)]
    peers += [(y, x, c, turned(z + d)) for d in (1, 2, 3)]
    peers += [(y, x, 1 - c, turned(z + d)) for d in (0, 1, 2, 3)]
    for device in peers:
        pl.semaphore_signal(barrier, inc=1, device_id=device, device_id_type=MESH)

    pair = pair_table(256, 128)

    def restrict(fine, index, scale):
        for k in range(2):
            total = scale * pooled(fine[2 * k] + fine[2 * k + 1], pair, half)
            own[index, k, pl.ds(16, 128), :] = total
            own[index, k, pl.ds(0, 16), :] = total[112:128]
            own[index, k, pl.ds(144, 16), :] = total[0:16]

    def restrict_last():
        load_p.wait()
        restrict(fine_p, 2, 0.125)

    pl.when(is_last)(restrict_last)
    load_s.wait()
    restrict(fine_s, 0, 0.0625)
    pl.semaphore_wait(barrier, len(peers))

    layers = pl.ds(2 * z, 2)
    rows = pl.ds(16 * c, 48)

    for d in (0, 1, 2, 3):
        to = turned(z + d)
        for core in (0, 1):
            if d or not core:
                send(
                    own.at[2, :, pl.ds(32 * to + 16 * core, 48), :], seed.at[layers],
                    seed_sem, (y, x, core, to), is_last,
                )

    def seed_self():
        seed[layers] = own[2, :, pl.ds(32 * z + 16, 48), :]

    pl.when(is_last)(seed_self)

    for d in (1, 3, 2):
        to = turned(z + d)
        send(
            own.at[0, :, pl.ds(32 * to, 64), :], buf.at[mine, layers], slot_sem.at[mine],
            (y, x, c, to),
        )
    buf[mine, layers] = own[0, :, pl.ds(32 * z, 64), :]
    load_r.wait()
    restrict(fine_r, 1, 0.0625)
    for d in (1, 3, 2):
        to = turned(z + d)
        send(
            own.at[1, :, pl.ds(32 * to + 16 * c, 48), :], rate_c.at[layers], rate_sem,
            (y, x, c, to),
        )
    rate_c[layers] = own[1, :, pl.ds(32 * z + 16 * c, 48), :]

    part = pl.ds(2 + 2 * c, 2)
    local = pltpu.make_async_copy(fine_p, restart.at[pl.ds(2, 4)], load_sem.at[0])

    def place_last():
        local.start()
        local.wait()

    send(fine_p.at[pl.ds(0, 2)], restart.at[pl.ds(2, 2)], restart_sem.at[0], partner, is_last)
    pl.when(is_last)(place_last)

    along = x * (1 - c) + y * c
    across = y * (1 - c) + x * c
    da, db = turned(along + 1), turned(across + 1)
    near = (db == 0) & ((da == 1) | (da == 3))
    side = (db == 1) | (db == 3)
    is_root = (da == 0) & (db == 0)

    class Item:
        def __init__(self, full, halves, sem):
            self.full, self.halves, self.sem = full, halves, sem

        def go(self, device, cond):
            send(self.full, self.full, self.sem, device, cond)

        def root(self, ready):
            ready()
            for device in (first(1), first(-1), second(1), second(-1)):
                self.go(device, is_root)

        def step_near(self):
            arrived(self.full, self.sem, near)
            view = self.halves(jnp.where(da == 1, 0, 1))
            send(view, view, self.sem, first(jnp.where(da == 1, 1, -1)), near)
            for step in (1, -1):
                self.go(second(step), near)

        def step_far(self):
            cond = (db == 0) & (da == 2)
            arrived(self.full, self.sem, cond)
            for step in (1, -1):
                self.go(second(step), cond)

        def step_side(self):
            arrived(self.full, self.sem, side)
            view = self.halves(jnp.where(db == 1, 0, 1))
            send(view, view, self.sem, second(jnp.where(db == 1, 1, -1)), side)

        def step_last(self):
            arrived(self.full, self.sem, db == 2)

    coarse_item = Item(seed, lambda h: seed.at[pl.ds(4 * h, 4)], seed_sem)
    fine_item = Item(
        restart.at[part], lambda h: restart.at[pl.ds(2 + 2 * c + h, 1)], restart_sem.at[0]
    )

    def seed_ready():
        arrived(seed.at[pl.ds(0, 6)], seed_sem, is_last)
        arrived(seed, seed_sem, mine == 30)

    coarse_item.root(seed_ready)

    for field, low, high, width, index in (
        (prev, prev_lo, prev_hi, 2, 0),
        (source, source_lo, source_hi, 1, 2),
        (rate, rate_lo, rate_hi, 1, 4),
    ):
        send(
            field.at[pl.ds(4 - width, width)], low, halo_sem.at[index], (y, x, c, turned(z + 1)),
            z < 3,
        )
        send(
            field.at[pl.ds(0, width)], high, halo_sem.at[index + 1], (y, x, c, turned(z - 1)),
            z > 0,
        )

    def chunk(da, db):
        return buf.at[slot(da, db)], slot_sem.at[slot(da, db)]

    def across_chip(da, db):
        view = buf.at[slot(da, db), :, pl.ds(16 * (1 - c), 48), :]
        send(view, view, slot_sem.at[slot(da, db)], partner)

    def onward(da, db):
        full, sem = chunk(da, db)
        for step in (1, -1):
            send(full, full, sem, second(step))
        across_chip(da, db)

    def relay(da, db, device, h):
        full, sem = chunk(da, db)
        arrived(full, sem)
        view = buf.at[slot(da, db), pl.ds(4 * h, 4)]
        send(view, view, sem, device)

    full, sem = chunk(0, 0)
    arrived(full.at[pl.ds(0, 6)], sem)
    for step in (1, -1):
        send(full, full, sem, first(step))
    onward(0, 0)
    fine_item.root(lambda: arrived(restart.at[part], restart_sem.at[0], mine == 30))
    relay(-1, 0, first(1), 0)
    onward(-1, 0)
    relay(1, 0, first(-1), 1)
    onward(1, 0)
    coarse_item.step_near()
    for step, h in ((-1, 0), (1, 1)):
        relay(0, step, second(-step), h)
        across_chip(0, step)
    arrived(*chunk(2, 0))
    onward(2, 0)
    coarse_item.step_far()
    fine_item.step_near()
    for a in (-1, 1):
        for step, h in ((-1, 0), (1, 1)):
            relay(a, step, second(-step), h)
            across_chip(a, step)
    arrived(*chunk(0, 2))
    across_chip(0, 2)
    coarse_item.step_side()
    for step, h in ((-1, 0), (1, 1)):
        relay(2, step, second(-step), h)
        across_chip(2, step)
    fine_item.step_far()
    for a in (-1, 1, 2):
        arrived(*chunk(a, 2))
        across_chip(a, 2)
    coarse_item.step_last()
    for a in range(4):
        for b in range(4):
            other = (a * 4 + b) * 2 + 1 - c
            arrived(buf.at[other, :, rows, :], slot_sem.at[other])
    arrived(rate_c.at[pl.ds(0, 6)], rate_sem)
    fine_item.step_side()

    state_a[...] = jnp.zeros_like(state_a)
    state_b[...] = jnp.zeros_like(state_b)
    state_a[pl.ds(1, 8), pl.ds(8, 48), :] = seed[...]
    inner = pl.ds(24, 16)
    up = (y, x, 1 - c, turned(z + c))
    down = (y, x, 1 - c, turned(z - 1 + c))

    def run(block, low, count, tiles):
        def body(i, carry):
            t = block * 8 + low + i

            def keep(ref, index):
                @pl.when(t >= 2 * chip)
                def _():
                    found[t - 2 * chip, index] = ref[:, inner, :]

            keep(state_a, 0)
            coarse_stage(state_a, state_b, rate_c, buf.at[t], 16 * c, tiles)
            keep(state_b, 1)
            coarse_stage(state_b, state_a, rate_c, buf.at[t], 16 * c, tiles)
            keep(state_a, 2)
            return carry

        lax.fori_loop(0, count, body, 0)

    for block in range(4):
        active = y >= block
        if block:
            e = block - 1

            def fill(e=e):
                edge_out[e] = state_a[pl.ds(1, 8), inner, :]

            pl.when(active)(fill)
            send(edge_out.at[e], edge_in.at[e, 0], edge_sem.at[e, 0], up, active)
            send(edge_out.at[e], edge_in.at[e, 1], edge_sem.at[e, 1], down, active)
            arrived(edge_in.at[e, 0], edge_sem.at[e, 0], active)
            arrived(edge_in.at[e, 1], edge_sem.at[e, 1], active)

            def spill(e=e):
                state_a[pl.ds(1, 8), pl.ds(8, 16), :] = edge_in[e, 0]
                state_a[pl.ds(1, 8), pl.ds(40, 16), :] = edge_in[e, 1]

            pl.when(active)(spill)
        count = jnp.where(y > block, 8, jnp.where(active, 2 * x + 2, 0))
        run(block, 0, jnp.minimum(count, 4), range(6))
        run(block, 4, jnp.maximum(count - 4, 0), range(1, 5))
        if block == 0:
            fine_item.step_last()
            own_part = restart.at[part]
            send(own_part, own_part, restart_sem.at[1], partner, mine != 30)
            send(
                restart.at[pl.ds(2, 2)], restart.at[pl.ds(6, 2)], restart_sem.at[2],
                (y, x, c, turned(z - 1)), (c == 0) & (z > 0),
            )
            send(
                restart.at[pl.ds(4, 2)], restart.at[pl.ds(0, 2)], restart_sem.at[2],
                (y, x, c, turned(z + 1)), (c == 1) & (z < 3),
            )

    for core in (0, 1):
        for d in (1, 3, 2, 0):
            to = turned(z + d)
            here = pl.ds(16 * slab, 16)
            send(
                found.at[core, :, pl.ds(2 * to, 4)], states.at[:, :, here, :], state_sem,
                (y, x, core, to), None if d else (c != core),
            )
    states[:, :, pl.ds(16 * slab, 16), :] = found[c, :, pl.ds(2 * z, 4)]

    halo_ready = ((c == 0) & (z < 3)) | ((c == 1) & (z > 0))
    halo = restart.at[pl.ds(6 - 6 * c, 2)]
    arrived(halo, restart_sem.at[2], halo_ready)
    send(halo, halo, restart_sem.at[3], partner, halo_ready)
    other_halo = ((c == 1) & (z < 3)) | ((c == 0) & (z > 0))
    arrived(restart.at[pl.ds(6 * c, 2)], restart_sem.at[3], other_halo)
    arrived(restart.at[pl.ds(4 - 2 * c, 2)], restart_sem.at[1], mine != 31)
    for index, view in enumerate((prev_lo, prev_hi, source_lo, source_hi, rate_lo, rate_hi)):
        arrived(view, halo_sem.at[index], (z > 0) if index % 2 == 0 else (z < 3))
    arrived(states.at[:, :, pl.ds(0, 112), :], state_sem)
    for cond, wait in waits:
        guarded(cond, wait)


def fine_kernel(
    prev, prev_lo, prev_hi, source, source_lo, source_hi, rate, rate_lo, rate_hi, restart, states,
    out,
    half, lifted, mixed, base, extra, last, later,
):
    z = lax.axis_index("space")
    w = stencil_weights(1.0)
    pair = pair_table(256, 128)
    spread = (
        lax.broadcasted_iota(jnp.int32, (128, 256), 0)
        == lax.broadcasted_iota(jnp.int32, (128, 256), 1) // 2
    ).astype(F32)

    def prev_layer(k):
        return prev_lo.at[k] if k < 2 else prev_hi.at[k - 6] if k > 5 else prev.at[k - 2]

    def of(low, middle, high, k):
        return low.at[0] if k < 2 else high.at[0] if k > 5 else middle.at[k - 2]

    def inside(k):
        return (z > 0) if k < 2 else (z < 3) if k > 5 else None

    def masked(k, value):
        cond = inside(k)
        return value if cond is None else jnp.where(cond, value, 0.0)

    for k in range(4):
        seed_c = 0.125 * pooled(restart[2 * k] + restart[2 * k + 1], pair, half)
        warm_c = 0.125 * pooled(
            prev_layer(2 * k)[...] + prev_layer(2 * k + 1)[...], pair, half
        )
        for n in range(3):
            change = states[n, k] - (warm_c if n else seed_c)
            wide = jnp.dot(
                change, spread, precision=lax.Precision.HIGHEST, preferred_element_type=F32
            )
            for h in range(2):
                column = wide[:, 128 * h : 128 * h + 128]
                lifted[n, k, h, pl.ds(0, 128, stride=2), :] = column
                lifted[n, k, h, pl.ds(1, 128, stride=2), :] = column

    def share(v):
        return v * pl.reciprocal(1.0 + v * v)

    def put(ref, k, i, value):
        ref[k, pl.ds(8 + 8 * i, 8), :] = value

    def guesses(i, carry):
        r = pl.ds(8 * i, 8)
        for k in range(8):
            lift = [
                jnp.concatenate([lifted[n, k // 2, h, r, :] for h in range(2)], axis=-1)
                for n in range(3)
            ]
            warm = prev_layer(k)[r, :]
            g = [masked(k, v) for v in (restart[k, r, :] + lift[0], warm + lift[1], warm + lift[2])]
            put(mixed, k, i, weights_one[0] * g[0] + weights_one[1] * g[1] + weights_one[2] * g[2])
            if 1 <= k <= 6:
                s = [share(v) for v in g]
                c = of(rate_lo, rate, rate_hi, k)[r, :]
                q = 0.5 * of(source_lo, source, source_hi, k)[r, :]
                base[k - 1, r, :] = (
                    g[0]
                    + c * (weights_one[0] * s[0] + weights_one[1] * s[1] + weights_one[2] * s[2])
                    + q
                )
                extra[k - 1, r, :] = (
                    weights_two[0] * g[0] + (weights_two[1] - 0.5) * g[1] + weights_two[2] * g[2]
                )
                if 2 <= k <= 5:
                    last[k - 2, r, :] = q + c * (
                        weights_two[0] * s[0]
                        + (weights_two[1] - 0.5) * s[1]
                        + weights_two[2] * s[2]
                    )
        return carry

    def wrap(ref, count):
        for k in range(count):
            ref[k, pl.ds(0, 8), :] = ref[k, pl.ds(256, 8), :]
            ref[k, pl.ds(264, 8), :] = ref[k, pl.ds(8, 8), :]

    def linear(ref, k, i, below, here, above):
        r = 8 * i + 8
        value = w[0] * here + w[1] * above + w[2] * below
        rows = ref[k, pl.ds(r - 8, 24), :]
        value += w[3] * rows[9:17] + w[4] * rows[7:15]
        return value + w[5] * pltpu.roll(here, 255, 1) + w[6] * pltpu.roll(here, 1, 1)

    lax.fori_loop(0, 32, guesses, 0)
    wrap(mixed, 8)

    def node_one(i, carry):
        r = pl.ds(8 * i, 8)
        planes = [mixed[k, pl.ds(8 + 8 * i, 8), :] for k in range(8)]
        for k in range(6):
            value = base[k, r, :] + linear(mixed, k + 1, i, *planes[k : k + 3])
            value = masked(0, value) if k == 0 else masked(7, value) if k == 5 else value
            if 1 <= k <= 4:
                out[0, 0, k - 1, r, :] = value
            put(later, k, i, 0.5 * value + extra[k, r, :])
        return carry

    lax.fori_loop(0, 32, node_one, 0)
    wrap(later, 6)

    def node_two(i, carry):
        r = pl.ds(8 * i, 8)
        planes = [later[k, pl.ds(8 + 8 * i, 8), :] for k in range(6)]
        for k in range(4):
            one = out[0, 0, k, r, :]
            value = one + 0.5 * rate[k, r, :] * share(one) + last[k, r, :]
            out[0, 1, k, r, :] = value + linear(later, k + 1, i, *planes[k : k + 3])
        return carry

    lax.fori_loop(0, 32, node_two, 0)


def shards(previous_end, source, rate):
    prev = previous_end[0]
    own = source[0]
    any_space = pl.BlockSpec(memory_space=pl.ANY)
    vmem = pl.BlockSpec(memory_space=pltpu.VMEM)
    dma = pltpu.SemaphoreType.DMA

    def shape(*dims):
        return jax.ShapeDtypeStruct(dims, F32)

    def scratch(*dims):
        return pltpu.VMEM(dims, F32)

    states, restart, *halos = pl.pallas_call(
        chain_kernel,
        out_shape=[shape(3, 4, 128, 128), shape(8, 256, 256)]
        + [shape(2, 256, 256)] * 2
        + [shape(1, 256, 256)] * 4,
        in_specs=[any_space] * 3,
        out_specs=[vmem] + [any_space] * 7,
        scratch_shapes=[
            scratch(4, 256, 256), scratch(4, 256, 256), scratch(4, 256, 256), scratch(256, 128),
            scratch(3, 2, 160, 128), scratch(32, 8, 64, 128), scratch(8, 48, 128),
            scratch(8, 48, 128), scratch(10, 64, 128), scratch(10, 64, 128),
            scratch(3, 8, 16, 128), scratch(3, 2, 8, 16, 128), scratch(2, 3, 10, 16, 128),
            dma((3,)), dma((N_SEND,)), dma((32,)), dma, dma, dma((3, 2)), dma, dma((6,)),
            dma((4,)),
        ],
        compiler_params=pltpu.CompilerParams(
            collective_id=0, has_side_effects=True, vmem_limit_bytes=40 * 1024 * 1024
        ),
    )(prev, own, rate)
    prev_lo, prev_hi, source_lo, source_hi, rate_lo, rate_hi = halos
    return pl.pallas_call(
        fine_kernel,
        out_shape=shape(1, 2, 4, 256, 256),
        in_specs=[vmem] * 11,
        out_specs=vmem,
        scratch_shapes=[
            scratch(256, 128), scratch(3, 4, 2, 256, 128), scratch(8, 272, 256),
            scratch(6, 256, 256), scratch(6, 256, 256), scratch(4, 256, 256),
            scratch(6, 272, 256),
        ],
        compiler_params=pltpu.CompilerParams(vmem_limit_bytes=48 * 1024 * 1024),
    )(prev, prev_lo, prev_hi, own, source_lo, source_hi, rate, rate_lo, rate_hi, restart, states)


def solution(mesh):
    torus = Mesh(
        mesh.devices.reshape(4, 4, 2, mesh.shape["space"]), ("tm_0", "tm_1", "tm_2", "space")
    )
    placed = (P(TM, "space", None, None), P(TM, "space", None, None), P("space", None, None))
    return jax.shard_map(
        shards,
        mesh=torus,
        in_specs=placed,
        out_specs=P(TM, None, "space", None, None),
        check_vma=False,
    )
```

```python
import jax
import jax.numpy as jnp
from jax import lax
from jax.experimental import pallas as pl
from jax.experimental.pallas import tpu as pltpu
from jax.sharding import Mesh
from jax.sharding import PartitionSpec as P

TM = ("tm_0", "tm_1", "tm_2")
AXES = TM + ("space",)
MESH = pl.DeviceIdType.MESH
F32 = jnp.float32

diffusion = 0.1
speed_z = 0.4
speed_x = 0.3
speed_y = 0.2
weights_one = (5.0 / 24.0, 1.0 / 3.0, -1.0 / 24.0)
weights_two = (-1.0 / 24.0, 1.0 / 3.0, 5.0 / 24.0)


def stencil_weights(spacing):
    d = diffusion / (spacing * spacing)
    out = [-6.0 * d]
    for speed in (speed_z, speed_x, speed_y):
        out += [d - speed / (2.0 * spacing), d + speed / (2.0 * spacing)]
    return out


def pair_table(fine, coarse):
    rows = lax.broadcasted_iota(jnp.int32, (fine, coarse), 0) // 2
    columns = lax.broadcasted_iota(jnp.int32, (fine, coarse), 1)
    return (rows == columns).astype(F32)


def pooled(total, pair, scratch):
    scratch[...] = jnp.dot(
        total, pair, precision=lax.Precision.HIGHEST, preferred_element_type=F32
    )
    return scratch[pl.ds(0, 128, stride=2), :] + scratch[pl.ds(1, 128, stride=2), :]


def coarse_stage(src, dst, rate, source, row, tiles):
    w = [0.5 * v for v in stencil_weights(2.0)]
    for j in tiles:
        r = 8 + 8 * j
        below = src[0, pl.ds(r, 8), :]
        here = src[1, pl.ds(r, 8), :]
        for k in range(1, 9):
            above = src[k + 1, pl.ds(r, 8), :]
            out = (1.0 + w[0]) * here + source[k - 1, pl.ds(row + 8 * j, 8), :]
            out += w[1] * above + w[2] * below
            out += w[3] * src[k, pl.ds(r + 1, 8), :] + w[4] * src[k, pl.ds(r - 1, 8), :]
            out += w[5] * pltpu.roll(here, 127, 1) + w[6] * pltpu.roll(here, 1, 1)
            out += rate[k - 1, pl.ds(8 * j, 8), :] * here * pl.reciprocal(1.0 + here * here)
            dst[k, pl.ds(r, 8), :] = out
            below, here = here, above


N_SEND = 256


def chain_kernel(
    prev, source, rate,
    states, restart, prev_lo, prev_hi, source_lo, source_hi, rate_lo, rate_hi,
    fine_s, fine_r, fine_p, half, own, buf, rate_c, seed, state_a, state_b,
    edge_out, edge_in, found,
    layer,
    load_sem, send_sem, slot_sem, fine_sem, seed_sem, rate_sem, edge_sem, state_sem, halo_sem,
    restart_sem,
):
    y, x, c, z = (lax.axis_index(name) for name in AXES)
    chip = y * 4 + x
    mine = chip * 2 + c
    slab = 2 * z + c
    is_last = mine == 31
    partner = (y, x, 1 - c, z)
    waits = []

    def guarded(cond, action):
        if cond is None:
            action()
        else:
            pl.when(cond)(action)

    def send(src, dst, sem, device, cond=None):
        index = len(waits)

        def build():
            return pltpu.make_async_remote_copy(
                src_ref=src, dst_ref=dst, send_sem=send_sem.at[index], recv_sem=sem,
                device_id=device, device_id_type=MESH,
            )

        waits.append((cond, lambda: build().wait_send()))
        guarded(cond, lambda: build().start())

    def arrived(view, sem, cond=None):
        def wait():
            pltpu.make_async_remote_copy(
                src_ref=view, dst_ref=view, send_sem=send_sem.at[0], recv_sem=sem,
                device_id=partner, device_id_type=MESH,
            ).wait_recv()

        guarded(cond, wait)

    def turned(value):
        return lax.rem(value + 8, 4)

    def first(step):
        return (turned(y + step * c), turned(x + step * (1 - c)), c, z)

    def second(step):
        return (turned(y + step * (1 - c)), turned(x + step * c), c, z)

    def slot(da, db):
        return (turned(y + da * c + db * (1 - c)) * 4 + turned(x + da * (1 - c) + db * c)) * 2 + c

    load_p = pltpu.make_async_copy(prev, fine_p, load_sem.at[0])
    load_s = pltpu.make_async_copy(source, fine_s, load_sem.at[1])
    load_r = pltpu.make_async_copy(rate, fine_r, load_sem.at[2])
    pl.when(is_last)(load_p.start)
    load_s.start()
    load_r.start()
    barrier = pltpu.get_barrier_semaphore()
    peers = [step(d) for step in (first, second) for d in (1, -1, 2)]
    peers += [(y, x, c, turned(z + d)) for d in (1, 2, 3)]
    peers += [(y, x, 1 - c, turned(z + d)) for d in (0, 1, 2, 3)]
    for device in peers:
        pl.semaphore_signal(barrier, inc=1, device_id=device, device_id_type=MESH)

    @pl.when(jnp.logical_not(is_last))
    def _():
        pl.semaphore_signal(barrier, inc=1, device_id=(3, 3, 1, z), device_id_type=MESH)

    pair = pair_table(256, 128)

    def restrict(fine, index, scale):
        for k in range(2):
            total = scale * pooled(fine[2 * k] + fine[2 * k + 1], pair, half)
            own[index, k, pl.ds(16, 128), :] = total
            own[index, k, pl.ds(0, 16), :] = total[112:128]
            own[index, k, pl.ds(144, 16), :] = total[0:16]

    def restrict_last():
        load_p.wait()
        restrict(fine_p, 2, 0.125)

    pl.when(is_last)(restrict_last)
    load_s.wait()
    restrict(fine_s, 0, 0.0625)
    pl.semaphore_wait(barrier, jnp.where(is_last, len(peers) + 31, len(peers)))

    layers = pl.ds(2 * z, 2)
    rows = pl.ds(16 * c, 48)
    along = x * (1 - c) + y * c
    across = y * (1 - c) + x * c
    in_line = across == 3
    is_root = in_line & (along == 3)

    send(own.at[2, 1], layer, seed_sem.at[0], partner, is_last)

    def seed_self():
        layer[...] = own[2, 0]

    pl.when(is_last)(seed_self)

    for d in (1, 3, 2):
        to = turned(z + d)
        send(
            own.at[0, :, pl.ds(32 * to, 64), :], buf.at[mine, layers], slot_sem.at[mine],
            (y, x, c, to),
        )
    buf[mine, layers] = own[0, :, pl.ds(32 * z, 64), :]
    arrived(layer, seed_sem.at[0], mine == 30)
    for d in (2, 1, -1):
        send(layer, layer, seed_sem.at[0], first(d), is_root)

    for n in range(31):
        send(
            fine_p.at[:, pl.ds(8 * n, 8), :], restart.at[pl.ds(2, 4), n // 2, n % 2],
            fine_sem.at[n], (n // 8, n // 2 % 4, n % 2, z), is_last,
        )

    @pl.when(is_last)
    def _():
        local = pltpu.make_async_copy(
            fine_p.at[:, pl.ds(248, 8), :], restart.at[pl.ds(2, 4), 15, 1], load_sem.at[0]
        )
        local.start()
        local.wait()

    load_r.wait()
    restrict(fine_r, 1, 0.0625)
    for d in (1, 3, 2):
        to = turned(z + d)
        send(
            own.at[1, :, pl.ds(32 * to + 16 * c, 48), :], rate_c.at[layers], rate_sem,
            (y, x, c, to),
        )
    rate_c[layers] = own[1, :, pl.ds(32 * z + 16 * c, 48), :]
    arrived(layer, seed_sem.at[0], in_line & (along != 3))
    for d in (2, 1, -1):
        send(layer, layer, seed_sem.at[0], second(d), in_line)

    def spread_seed():
        arrived(layer, seed_sem.at[0], jnp.logical_not(in_line))
        target = 2 * z + 1 - c
        for d in (1, 3, 2, 0):
            for core in (0, 1):
                to = turned(z + d)
                view = layer.at[pl.ds(32 * to + 16 * core, 48), :]
                cond = None if d else (c != core)
                send(view, seed.at[target], seed_sem.at[1], (y, x, core, to), cond)
        seed[target] = layer[pl.ds(32 * z + 16 * c, 48), :]

    for field, low, high, width, index in (
        (prev, prev_lo, prev_hi, 2, 0),
        (source, source_lo, source_hi, 1, 2),
        (rate, rate_lo, rate_hi, 1, 4),
    ):
        send(
            field.at[pl.ds(4 - width, width)], low, halo_sem.at[index], (y, x, c, turned(z + 1)),
            z < 3,
        )
        send(
            field.at[pl.ds(0, width)], high, halo_sem.at[index + 1], (y, x, c, turned(z - 1)),
            z > 0,
        )

    def chunk(da, db):
        return buf.at[slot(da, db)], slot_sem.at[slot(da, db)]

    def across_chip(da, db):
        view = buf.at[slot(da, db), :, pl.ds(16 * (1 - c), 48), :]
        send(view, view, slot_sem.at[slot(da, db)], partner)

    def onward(da, db):
        full, sem = chunk(da, db)
        for step in (1, -1):
            send(full, full, sem, second(step))
        across_chip(da, db)

    def relay(da, db, device, h):
        full, sem = chunk(da, db)
        arrived(full, sem)
        view = buf.at[slot(da, db), pl.ds(4 * h, 4)]
        send(view, view, sem, device)

    def fine(da, db):
        here = slot(da, db)
        return restart.at[pl.ds(2, 4), here // 2, c], fine_sem.at[here]

    def fine_onward(da, db):
        full, sem = fine(da, db)
        for step in (1, -1):
            send(full, full, sem, second(step))

    def fine_relay(da, db, device, h):
        full, sem = fine(da, db)
        arrived(full, sem)
        view = restart.at[pl.ds(2 + 2 * h, 2), slot(da, db) // 2, c]
        send(view, view, sem, device)

    def fine_own():
        full, sem = fine(0, 0)
        arrived(full, sem, jnp.logical_not(is_last))
        for step in (1, -1):
            send(full, full, sem, first(step))
        fine_onward(0, 0)

    def near(relay, onward):
        relay(-1, 0, first(1), 0)
        onward(-1, 0)
        relay(1, 0, first(-1), 1)
        onward(1, 0)

    def ring(relay, a):
        for step, h in ((-1, 0), (1, 1)):
            relay(a, step, second(-step), h)
            if relay is not fine_relay:
                across_chip(a, step)

    full, sem = chunk(0, 0)
    arrived(full.at[pl.ds(0, 6)], sem)
    for step in (1, -1):
        send(full, full, sem, first(step))
    onward(0, 0)
    fine_own()
    near(relay, onward)
    spread_seed()
    ring(relay, 0)
    near(fine_relay, fine_onward)
    arrived(*chunk(2, 0))
    onward(2, 0)
    ring(relay, -1)
    ring(relay, 1)
    ring(fine_relay, 0)
    arrived(*fine(2, 0))
    fine_onward(2, 0)
    arrived(*chunk(0, 2))
    across_chip(0, 2)
    ring(relay, 2)
    ring(fine_relay, -1)
    ring(fine_relay, 1)
    for a in (-1, 1, 2):
        arrived(*chunk(a, 2))
        across_chip(a, 2)
    ring(fine_relay, 2)
    for a in range(4):
        for b in range(4):
            other = (a * 4 + b) * 2 + 1 - c
            arrived(buf.at[other, :, rows, :], slot_sem.at[other])
    arrived(rate_c.at[pl.ds(0, 6)], rate_sem)
    arrived(seed.at[pl.ds(0, 7)], seed_sem.at[1])

    state_a[...] = jnp.zeros_like(state_a)
    state_b[...] = jnp.zeros_like(state_b)
    state_a[pl.ds(1, 8), pl.ds(8, 48), :] = seed[...]
    inner = pl.ds(24, 16)
    up = (y, x, 1 - c, turned(z + c))
    down = (y, x, 1 - c, turned(z - 1 + c))

    def run(block, low, count, tiles):
        def body(i, carry):
            t = block * 8 + low + i

            def keep(ref, index):
                @pl.when(t >= 2 * chip)
                def _():
                    found[t - 2 * chip, index] = ref[:, inner, :]

            keep(state_a, 0)
            coarse_stage(state_a, state_b, rate_c, buf.at[t], 16 * c, tiles)
            keep(state_b, 1)
            coarse_stage(state_b, state_a, rate_c, buf.at[t], 16 * c, tiles)
            keep(state_a, 2)
            return carry

        lax.fori_loop(0, count, body, 0)

    for block in range(4):
        active = y >= block
        if block:
            e = block - 1

            def fill(e=e):
                edge_out[e] = state_a[pl.ds(1, 8), inner, :]

            pl.when(active)(fill)
            send(edge_out.at[e], edge_in.at[e, 0], edge_sem.at[e, 0], up, active)
            send(edge_out.at[e], edge_in.at[e, 1], edge_sem.at[e, 1], down, active)
            arrived(edge_in.at[e, 0], edge_sem.at[e, 0], active)
            arrived(edge_in.at[e, 1], edge_sem.at[e, 1], active)

            def spill(e=e):
                state_a[pl.ds(1, 8), pl.ds(8, 16), :] = edge_in[e, 0]
                state_a[pl.ds(1, 8), pl.ds(40, 16), :] = edge_in[e, 1]

            pl.when(active)(spill)
        count = jnp.where(y > block, 8, jnp.where(active, 2 * x + 2, 0))
        run(block, 0, jnp.minimum(count, 4), range(6))
        run(block, 4, jnp.maximum(count - 4, 0), range(1, 5))
        if block == 0:
            for a in (0, -1, 1, 2):
                arrived(*fine(a, 2))
            view = restart.at[pl.ds(2, 4), :, c]
            send(view, view, restart_sem.at[0], partner)
            for low, to, step, index in ((2, 6, -1, 1), (4, 0, 1, 2)):
                send(
                    restart.at[pl.ds(low, 2), :, c], restart.at[pl.ds(to, 2), :, c],
                    restart_sem.at[index], (y, x, c, turned(z + step)),
                    (z > 0) if step < 0 else (z < 3),
                )

    for core in (0, 1):
        for d in (1, 3, 2, 0):
            to = turned(z + d)
            here = pl.ds(16 * slab, 16)
            send(
                found.at[core, :, pl.ds(2 * to, 4)], states.at[:, :, here, :], state_sem,
                (y, x, core, to), None if d else (c != core),
            )
    states[:, :, pl.ds(16 * slab, 16), :] = found[c, :, pl.ds(2 * z, 4)]

    for low, index, cond in ((6, 1, z < 3), (0, 2, z > 0)):
        view = restart.at[pl.ds(low, 2), :, c]
        arrived(view, restart_sem.at[index], cond)
        send(view, view, restart_sem.at[index + 2], partner, cond)
    for low, index, cond in ((6, 3, z < 3), (0, 4, z > 0)):
        arrived(restart.at[pl.ds(low, 2), :, 1 - c], restart_sem.at[index], cond)
    arrived(restart.at[pl.ds(2, 4), :, 1 - c], restart_sem.at[0])
    for index, view in enumerate((prev_lo, prev_hi, source_lo, source_hi, rate_lo, rate_hi)):
        arrived(view, halo_sem.at[index], (z > 0) if index % 2 == 0 else (z < 3))
    arrived(states.at[:, :, pl.ds(0, 112), :], state_sem)
    for cond, wait in waits:
        guarded(cond, wait)


def fine_kernel(*refs):
    inputs, out = refs[:11], refs[11]
    half, lifted, mixed, base, extra, last, later = refs[12:19]
    held, load_sem = refs[19:30], refs[30]
    loads = [
        pltpu.make_async_copy(a, b, load_sem.at[n]) for n, (a, b) in enumerate(zip(inputs, held))
    ]
    for n in (10, 9, 0, 1, 2, 3, 4, 5, 6, 7, 8):
        loads[n].start()
    prev, prev_lo, prev_hi, source, source_lo, source_hi, rate, rate_lo, rate_hi, restart, states = held
    z = lax.axis_index("space")
    w = stencil_weights(1.0)
    pair = pair_table(256, 128)
    spread = (
        lax.broadcasted_iota(jnp.int32, (128, 256), 0)
        == lax.broadcasted_iota(jnp.int32, (128, 256), 1) // 2
    ).astype(F32)

    def prev_layer(k):
        return prev_lo.at[k] if k < 2 else prev_hi.at[k - 6] if k > 5 else prev.at[k - 2]

    def of(low, middle, high, k):
        return low.at[0] if k < 2 else high.at[0] if k > 5 else middle.at[k - 2]

    def inside(k):
        return (z > 0) if k < 2 else (z < 3) if k > 5 else None

    def masked(k, value):
        cond = inside(k)
        return value if cond is None else jnp.where(cond, value, 0.0)

    for n in (10, 9, 0, 1, 2):
        loads[n].wait()
    for k in range(4):
        seed_c = 0.125 * pooled(restart[2 * k] + restart[2 * k + 1], pair, half)
        warm_c = 0.125 * pooled(
            prev_layer(2 * k)[...] + prev_layer(2 * k + 1)[...], pair, half
        )
        for n in range(3):
            change = states[n, k] - (warm_c if n else seed_c)
            wide = jnp.dot(
                change, spread, precision=lax.Precision.HIGHEST, preferred_element_type=F32
            )
            for h in range(2):
                column = wide[:, 128 * h : 128 * h + 128]
                lifted[n, k, h, pl.ds(0, 128, stride=2), :] = column
                lifted[n, k, h, pl.ds(1, 128, stride=2), :] = column

    def share(v):
        return v * pl.reciprocal(1.0 + v * v)

    def put(ref, k, i, value):
        for h in range(2):
            ref[k, h, pl.ds(8 + 8 * i, 8), :] = value[:, 128 * h : 128 * h + 128]

    def row(ref, k, start):
        return jnp.concatenate([ref[k, h, pl.ds(start, 8), :] for h in range(2)], axis=-1)

    def guesses(i, carry):
        r = pl.ds(8 * i, 8)
        for k in range(8):
            lift = [
                jnp.concatenate([lifted[n, k // 2, h, r, :] for h in range(2)], axis=-1)
                for n in range(3)
            ]
            warm = prev_layer(k)[r, :]
            g = [masked(k, v) for v in (restart[k, r, :] + lift[0], warm + lift[1], warm + lift[2])]
            put(mixed, k, i, weights_one[0] * g[0] + weights_one[1] * g[1] + weights_one[2] * g[2])
            if 1 <= k <= 6:
                s = [share(v) for v in g]
                c = of(rate_lo, rate, rate_hi, k)[r, :]
                q = 0.5 * of(source_lo, source, source_hi, k)[r, :]
                base[k - 1, r, :] = (
                    g[0]
                    + c * (weights_one[0] * s[0] + weights_one[1] * s[1] + weights_one[2] * s[2])
                    + q
                )
                extra[k - 1, r, :] = (
                    weights_two[0] * g[0] + (weights_two[1] - 0.5) * g[1] + weights_two[2] * g[2]
                )
                if 2 <= k <= 5:
                    last[k - 2, r, :] = q + c * (
                        weights_two[0] * s[0]
                        + (weights_two[1] - 0.5) * s[1]
                        + weights_two[2] * s[2]
                    )
        return carry

    def wrap(ref, count):
        for k in range(count):
            for h in range(2):
                ref[k, h, pl.ds(0, 8), :] = ref[k, h, pl.ds(256, 8), :]
                ref[k, h, pl.ds(264, 8), :] = ref[k, h, pl.ds(8, 8), :]

    def linear(ref, k, i, below, here, above):
        r = 8 * i + 8
        value = w[0] * here + w[1] * above + w[2] * below
        value += w[3] * row(ref, k, r + 1) + w[4] * row(ref, k, r - 1)
        return value + w[5] * pltpu.roll(here, 255, 1) + w[6] * pltpu.roll(here, 1, 1)

    for n in range(3, 9):
        loads[n].wait()
    lax.fori_loop(0, 32, guesses, 0, unroll=2)
    wrap(mixed, 8)

    def node_one(i, carry):
        r = pl.ds(8 * i, 8)
        planes = [row(mixed, k, 8 + 8 * i) for k in range(8)]
        for k in range(6):
            value = base[k, r, :] + linear(mixed, k + 1, i, *planes[k : k + 3])
            value = masked(0, value) if k == 0 else masked(7, value) if k == 5 else value
            if 1 <= k <= 4:
                out[0, 0, k - 1, r, :] = value
            put(later, k, i, 0.5 * value + extra[k, r, :])
        return carry

    lax.fori_loop(0, 32, node_one, 0, unroll=4)
    wrap(later, 6)

    def node_two(i, carry):
        r = pl.ds(8 * i, 8)
        planes = [row(later, k, 8 + 8 * i) for k in range(6)]
        for k in range(4):
            one = out[0, 0, k, r, :]
            value = one + 0.5 * rate[k, r, :] * share(one) + last[k, r, :]
            out[0, 1, k, r, :] = value + linear(later, k + 1, i, *planes[k : k + 3])
        return carry

    lax.fori_loop(0, 32, node_two, 0, unroll=4)


def shards(previous_end, source, rate):
    prev = previous_end[0]
    own = source[0]
    any_space = pl.BlockSpec(memory_space=pl.ANY)
    vmem = pl.BlockSpec(memory_space=pltpu.VMEM)
    dma = pltpu.SemaphoreType.DMA

    def shape(*dims):
        return jax.ShapeDtypeStruct(dims, F32)

    def scratch(*dims):
        return pltpu.VMEM(dims, F32)

    states, restart, *halos = pl.pallas_call(
        chain_kernel,
        out_shape=[shape(3, 4, 128, 128), shape(8, 16, 2, 8, 256)]
        + [shape(2, 256, 256)] * 2
        + [shape(1, 256, 256)] * 4,
        in_specs=[any_space] * 3,
        out_specs=[vmem] + [any_space] * 7,
        scratch_shapes=[
            scratch(4, 256, 256), scratch(4, 256, 256), scratch(4, 256, 256), scratch(256, 128),
            scratch(3, 2, 160, 128), scratch(32, 8, 64, 128), scratch(8, 48, 128),
            scratch(8, 48, 128), scratch(10, 64, 128), scratch(10, 64, 128),
            scratch(3, 8, 16, 128), scratch(3, 2, 8, 16, 128), scratch(2, 3, 10, 16, 128),
            scratch(160, 128),
            dma((3,)), dma((N_SEND,)), dma((32,)), dma((32,)), dma((2,)), dma, dma((3, 2)), dma,
            dma((6,)), dma((5,)),
        ],
        compiler_params=pltpu.CompilerParams(
            collective_id=0, has_side_effects=True, vmem_limit_bytes=63 * 1024 * 1024
        ),
    )(prev, own, rate)
    prev_lo, prev_hi, source_lo, source_hi, rate_lo, rate_hi = halos
    restart = restart.reshape(8, 256, 256)
    return pl.pallas_call(
        fine_kernel,
        out_shape=shape(1, 2, 4, 256, 256),
        in_specs=[any_space] * 11,
        out_specs=vmem,
        scratch_shapes=[
            scratch(256, 128), scratch(3, 4, 2, 256, 128), scratch(8, 2, 272, 128),
            scratch(6, 256, 256), scratch(6, 256, 256), scratch(4, 256, 256),
            scratch(6, 2, 272, 128),
            scratch(4, 256, 256), scratch(2, 256, 256), scratch(2, 256, 256),
            scratch(4, 256, 256), scratch(1, 256, 256), scratch(1, 256, 256),
            scratch(4, 256, 256), scratch(1, 256, 256), scratch(1, 256, 256),
            scratch(8, 256, 256), scratch(3, 4, 128, 128), dma((11,)),
        ],
        compiler_params=pltpu.CompilerParams(vmem_limit_bytes=63 * 1024 * 1024),
    )(prev, prev_lo, prev_hi, own, source_lo, source_hi, rate, rate_lo, rate_hi, restart, states)


def solution(mesh):
    torus = Mesh(
        mesh.devices.reshape(4, 4, 2, mesh.shape["space"]), ("tm_0", "tm_1", "tm_2", "space")
    )
    placed = (P(TM, "space", None, None), P(TM, "space", None, None), P("space", None, None))
    return jax.shard_map(
        shards,
        mesh=torus,
        in_specs=placed,
        out_specs=P(TM, None, "space", None, None),
        check_vma=False,
    )
```

```python
import jax
import jax.numpy as jnp
from jax import lax
from jax.experimental import pallas as pl
from jax.experimental.pallas import tpu as pltpu
from jax.sharding import Mesh
from jax.sharding import PartitionSpec as P

TM = ("tm_0", "tm_1", "tm_2")
AXES = TM + ("space",)
MESH = pl.DeviceIdType.MESH
F32 = jnp.float32

diffusion = 0.1
speed_z = 0.4
speed_x = 0.3
speed_y = 0.2
weights_one = (5.0 / 24.0, 1.0 / 3.0, -1.0 / 24.0)
weights_two = (-1.0 / 24.0, 1.0 / 3.0, 5.0 / 24.0)


def stencil_weights(spacing):
    d = diffusion / (spacing * spacing)
    out = [-6.0 * d]
    for speed in (speed_z, speed_x, speed_y):
        out += [d - speed / (2.0 * spacing), d + speed / (2.0 * spacing)]
    return out


def pair_table(fine, coarse):
    rows = lax.broadcasted_iota(jnp.int32, (fine, coarse), 0) // 2
    columns = lax.broadcasted_iota(jnp.int32, (fine, coarse), 1)
    return (rows == columns).astype(F32)


def pooled(total, pair, scratch):
    scratch[...] = jnp.dot(
        total, pair, precision=lax.Precision.HIGHEST, preferred_element_type=F32
    )
    return scratch[pl.ds(0, 128, stride=2), :] + scratch[pl.ds(1, 128, stride=2), :]


def coarse_stage(src, dst, planes, starts, at):
    w = [0.5 * v for v in stencil_weights(2.0)]
    for j, r in enumerate(starts):
        below = src[planes[0][0] - 1, pl.ds(r, 8), :]
        here = src[planes[0][0], pl.ds(r, 8), :]
        for k, to, n in planes:
            above = src[k + 1, pl.ds(r, 8), :]
            rate, source = at(n, j)
            out = (1.0 + w[0]) * here + source
            out += w[1] * above + w[2] * below
            out += w[3] * src[k, pl.ds(r + 1, 8), :] + w[4] * src[k, pl.ds(r - 1, 8), :]
            out += w[5] * pltpu.roll(here, 127, 1) + w[6] * pltpu.roll(here, 1, 1)
            out += rate * here * pl.reciprocal(1.0 + here * here)
            dst[to, pl.ds(r, 8), :] = out
            below, here = here, above


N_SEND = 256


def chain_kernel(
    prev, source, rate,
    states, restart, prev_lo, prev_hi, source_lo, source_hi, rate_lo, rate_hi,
    fine_s, fine_r, fine_p, half, own, buf, rate_c, seed, state_a, state_b,
    edge_out, edge_in, found, layer, start, mid, end_state, near_c, warm,
    load_sem, send_sem, slot_sem, fine_sem, seed_sem, rate_sem, edge_sem, state_sem, halo_sem,
    restart_sem, near_sem, halo_piece,
):
    y, x, c, z = (lax.axis_index(name) for name in AXES)
    chip = y * 4 + x
    mine = chip * 2 + c
    slab = 2 * z + c
    is_last = mine == 31
    partner = (y, x, 1 - c, z)
    waits = []

    def guarded(cond, action):
        if cond is None:
            action()
        else:
            pl.when(cond)(action)

    def send(src, dst, sem, device, cond=None):
        index = len(waits)

        def build():
            return pltpu.make_async_remote_copy(
                src_ref=src, dst_ref=dst, send_sem=send_sem.at[index], recv_sem=sem,
                device_id=device, device_id_type=MESH,
            )

        waits.append((cond, lambda: build().wait_send()))
        guarded(cond, lambda: build().start())

    def arrived(view, sem, cond=None):
        def wait():
            pltpu.make_async_remote_copy(
                src_ref=view, dst_ref=view, send_sem=send_sem.at[0], recv_sem=sem,
                device_id=partner, device_id_type=MESH,
            ).wait_recv()

        guarded(cond, wait)

    def turned(value):
        return lax.rem(value + 8, 4)

    def first(step):
        return (turned(y + step * c), turned(x + step * (1 - c)), c, z)

    def second(step):
        return (turned(y + step * (1 - c)), turned(x + step * c), c, z)

    def slot(da, db):
        return (turned(y + da * c + db * (1 - c)) * 4 + turned(x + da * (1 - c) + db * c)) * 2 + c

    load_p = pltpu.make_async_copy(prev, fine_p, load_sem.at[0])
    load_s = pltpu.make_async_copy(source, fine_s, load_sem.at[1])
    load_r = pltpu.make_async_copy(rate, fine_r, load_sem.at[2])
    load_p.start()
    load_s.start()
    load_r.start()
    barrier = pltpu.get_barrier_semaphore()
    peers = [step(d) for step in (first, second) for d in (1, -1, 2)]
    peers += [(y, x, c, turned(z + d)) for d in (1, 2, 3)]
    peers += [(y, x, 1 - c, turned(z + d)) for d in (0, 1, 2, 3)]
    for device in peers:
        pl.semaphore_signal(barrier, inc=1, device_id=device, device_id_type=MESH)

    @pl.when(jnp.logical_not(is_last))
    def _():
        pl.semaphore_signal(barrier, inc=1, device_id=(3, 3, 1, z), device_id_type=MESH)

    pair = pair_table(256, 128)

    def restrict(fine, index, scale):
        for k in range(2):
            total = scale * pooled(fine[2 * k] + fine[2 * k + 1], pair, half)
            own[index, k, pl.ds(16, 128), :] = total
            own[index, k, pl.ds(0, 16), :] = total[112:128]
            own[index, k, pl.ds(144, 16), :] = total[0:16]

    load_p.wait()
    pl.when(is_last)(lambda: restrict(fine_p, 2, 0.125))
    load_s.wait()
    restrict(fine_s, 0, 0.0625)
    pl.semaphore_wait(barrier, jnp.where(is_last, len(peers) + 31, len(peers)))

    layers = pl.ds(2 * z, 2)
    rows = pl.ds(16 * c, 48)
    along = x * (1 - c) + y * c
    across = y * (1 - c) + x * c
    in_line = across == 3
    is_root = in_line & (along == 3)

    send(own.at[2, 1], layer, seed_sem.at[0], partner, is_last)

    def seed_self():
        layer[...] = own[2, 0]

    pl.when(is_last)(seed_self)

    for d in (1, 3, 2):
        to = turned(z + d)
        send(
            own.at[0, :, pl.ds(32 * to, 64), :], buf.at[mine, layers], slot_sem.at[mine],
            (y, x, c, to),
        )
    buf[mine, layers] = own[0, :, pl.ds(32 * z, 64), :]
    arrived(layer, seed_sem.at[0], mine == 30)
    for d in (2, 1, -1):
        send(layer, layer, seed_sem.at[0], first(d), is_root)

    def fine_halo(field, low, high, width, index):
        send(
            field.at[pl.ds(4 - width, width)], low, halo_sem.at[index], (y, x, c, turned(z + 1)),
            z < 3,
        )
        send(
            field.at[pl.ds(0, width)], high, halo_sem.at[index + 1], (y, x, c, turned(z - 1)),
            z > 0,
        )

    def other_halos():
        for f in range(2):
            for n, step, cond in ((0, 1, z < 3), (1, -1, z > 0)):
                send(
                    own.at[f, :, pl.ds(16, 128), :], near_c.at[f, pl.ds(4 * n, 2)],
                    near_sem.at[f, n], (y, x, c, turned(z + step)), cond,
                )
        fine_halo(source, source_lo, source_hi, 1, 2)
        fine_halo(rate, rate_lo, rate_hi, 1, 4)

    fine_halo(prev, prev_lo, prev_hi, 2, 0)

    for n in range(31):
        send(
            fine_p.at[:, pl.ds(8 * n, 8), :], restart.at[pl.ds(2, 4), n // 2, n % 2],
            fine_sem.at[n], (n // 8, n // 2 % 4, n % 2, z), is_last,
        )

    @pl.when(is_last)
    def _():
        local = pltpu.make_async_copy(
            fine_p.at[:, pl.ds(248, 8), :], restart.at[pl.ds(2, 4), 15, 1], load_sem.at[0]
        )
        local.start()
        local.wait()

    load_r.wait()
    restrict(fine_r, 1, 0.0625)
    for d in (1, 3, 2):
        to = turned(z + d)
        send(
            own.at[1, :, pl.ds(32 * to + 16 * c, 48), :], rate_c.at[layers], rate_sem,
            (y, x, c, to),
        )
    rate_c[layers] = own[1, :, pl.ds(32 * z + 16 * c, 48), :]
    arrived(layer, seed_sem.at[0], in_line & (along != 3))
    for d in (2, 1, -1):
        send(layer, layer, seed_sem.at[0], second(d), in_line)

    def spread_seed():
        arrived(layer, seed_sem.at[0], jnp.logical_not(in_line))
        target = 2 * z + 1 - c
        for d in (1, 3, 2, 0):
            for core in (0, 1):
                to = turned(z + d)
                view = layer.at[pl.ds(32 * to + 16 * core, 48), :]
                cond = None if d else (c != core)
                send(view, seed.at[target], seed_sem.at[1], (y, x, core, to), cond)
        seed[target] = layer[pl.ds(32 * z + 16 * c, 48), :]

    def chunk(da, db):
        return buf.at[slot(da, db)], slot_sem.at[slot(da, db)]

    def across_chip(da, db):
        view = buf.at[slot(da, db), :, pl.ds(16 * (1 - c), 48), :]
        send(view, view, slot_sem.at[slot(da, db)], partner)

    def onward(da, db):
        full, sem = chunk(da, db)
        for step in (1, -1):
            send(full, full, sem, second(step))
        across_chip(da, db)

    def relay(da, db, device, h):
        full, sem = chunk(da, db)
        arrived(full, sem)
        view = buf.at[slot(da, db), pl.ds(4 * h, 4)]
        send(view, view, sem, device)

    def fine(da, db):
        here = slot(da, db)
        return restart.at[pl.ds(2, 4), here // 2, c], fine_sem.at[here]

    def fine_onward(da, db):
        full, sem = fine(da, db)
        for step in (1, -1):
            send(full, full, sem, second(step))

    def fine_relay(da, db, device, h):
        full, sem = fine(da, db)
        arrived(full, sem)
        view = restart.at[pl.ds(2 + 2 * h, 2), slot(da, db) // 2, c]
        send(view, view, sem, device)

    def fine_own():
        full, sem = fine(0, 0)
        arrived(full, sem, jnp.logical_not(is_last))
        for step in (1, -1):
            send(full, full, sem, first(step))
        fine_onward(0, 0)

    def near(relay, onward):
        relay(-1, 0, first(1), 0)
        onward(-1, 0)
        relay(1, 0, first(-1), 1)
        onward(1, 0)

    def ring(relay, a):
        for step, h in ((-1, 0), (1, 1)):
            relay(a, step, second(-step), h)
            if relay is not fine_relay:
                across_chip(a, step)

    full, sem = chunk(0, 0)
    arrived(full.at[pl.ds(0, 6)], sem)
    for step in (1, -1):
        send(full, full, sem, first(step))
    onward(0, 0)
    fine_own()
    near(relay, onward)
    spread_seed()
    other_halos()
    ring(relay, 0)
    near(fine_relay, fine_onward)
    arrived(*chunk(2, 0))
    onward(2, 0)
    ring(relay, -1)
    ring(relay, 1)
    ring(fine_relay, 0)
    arrived(*fine(2, 0))
    fine_onward(2, 0)
    arrived(*chunk(0, 2))
    across_chip(0, 2)
    ring(relay, 2)
    for a in (-1, 1, 2):
        arrived(*chunk(a, 2))
        across_chip(a, 2)
    for a in range(4):
        for b in range(4):
            other = (a * 4 + b) * 2 + 1 - c
            arrived(buf.at[other, :, rows, :], slot_sem.at[other])
    arrived(rate_c.at[pl.ds(0, 6)], rate_sem)
    arrived(seed.at[pl.ds(0, 7)], seed_sem.at[1])

    state_a[...] = jnp.zeros_like(state_a)
    state_b[...] = jnp.zeros_like(state_b)
    state_a[pl.ds(1, 8), pl.ds(8, 48), :] = seed[...]
    inner = pl.ds(24, 16)
    up = (y, x, 1 - c, turned(z + c))
    down = (y, x, 1 - c, turned(z - 1 + c))

    def run(block, low, count, tiles):
        def body(i, carry):
            t = block * 8 + low + i

            @pl.when(t == 2 * chip)
            def _():
                found[0] = state_a[pl.ds(1, 8), inner, :]

            def at(n, j):
                r = 8 * tiles[j]
                return rate_c[n, pl.ds(r, 8), :], buf[t, n, pl.ds(16 * c + r, 8), :]

            planes = [(k, k, k - 1) for k in range(1, 9)]
            starts = [8 + 8 * tile for tile in tiles]
            coarse_stage(state_a, state_b, planes, starts, at)
            coarse_stage(state_b, state_a, planes, starts, at)
            return carry

        lax.fori_loop(0, count, body, 0)

    for block in range(4):
        active = y >= block
        if block:
            e = block - 1

            def fill(e=e):
                edge_out[e] = state_a[pl.ds(1, 8), inner, :]

            pl.when(active)(fill)
            send(edge_out.at[e], edge_in.at[e, 0], edge_sem.at[e, 0], up, active)
            send(edge_out.at[e], edge_in.at[e, 1], edge_sem.at[e, 1], down, active)
            if block == 1:
                for a in (-1, 1, 2):
                    ring(fine_relay, a)
                for a in (0, -1, 1, 2):
                    arrived(*fine(a, 2))
                view = restart.at[pl.ds(2, 4), :, c]
                send(view, view, restart_sem.at[0], partner)
            for piece in ((0,), (1, 2), (3,))[e]:
                for low, to, step, index in ((2, 6, -1, 1), (4, 0, 1, 2)):
                    some = pl.ds(4 * piece, 4)
                    send(
                        restart.at[pl.ds(low, 2), some, c], restart.at[pl.ds(to, 2), some, c],
                        halo_piece.at[index - 1, piece], (y, x, c, turned(z + step)),
                        (z > 0) if step < 0 else (z < 3),
                    )
            arrived(edge_in.at[e, 0], edge_sem.at[e, 0], active)
            arrived(edge_in.at[e, 1], edge_sem.at[e, 1], active)

            def spill(e=e):
                state_a[pl.ds(1, 8), pl.ds(8, 16), :] = edge_in[e, 0]
                state_a[pl.ds(1, 8), pl.ds(40, 16), :] = edge_in[e, 1]

            pl.when(active)(spill)
        count = jnp.where(y > block, 8, jnp.where(active, 2 * x + 1, 0))
        run(block, 0, jnp.minimum(count, 4), range(6))
        run(block, 4, jnp.maximum(count - 4, 0), range(1, 5))

    found[1] = state_a[pl.ds(1, 8), inner, :]
    here = pl.ds(8 + 16 * slab, 16)
    for d in (1, 3, 2, 0):
        to = turned(z + d)
        end = (to == 0) | (to == 3)
        for core in (0, 1):
            for count, low, cond in (
                (5, jnp.where(to == 0, 0, 3), end),
                (7, jnp.where(to == 1, 0, 1), jnp.logical_not(end)),
            ):
                send(
                    found.at[core, pl.ds(low, count)], start.at[pl.ds(3 + low, count), here, :],
                    state_sem, (y, x, core, to), cond if d else cond & (c != core),
                )
    zero = jnp.zeros((3, 144, 128), F32)
    start[pl.ds(0, 3)] = zero
    start[pl.ds(11, 3)] = zero
    start[pl.ds(3, 8), here, :] = found[c]

    for index in (0, 1):
        arrived((prev_lo, prev_hi)[index], halo_sem.at[index], (z < 3) if index else (z > 0))
    sides = [
        pltpu.make_async_copy(view, fine_r.at[pl.ds(2 * n, 2)], load_sem.at[1 + n])
        for n, view in enumerate((prev_lo, prev_hi))
    ]
    for copy in sides:
        copy.start()
    for n in range(2):
        warm[1 + n] = 0.125 * pooled(fine_p[2 * n] + fine_p[2 * n + 1], pair, half)
    for copy in sides:
        copy.wait()
    for n in range(2):
        warm[3 * n] = 0.125 * pooled(fine_r[2 * n] + fine_r[2 * n + 1], pair, half)
    for f in range(2):
        near_c[f, pl.ds(2, 2)] = own[f, :, pl.ds(16, 128), :]
        for n, cond in ((0, z > 0), (1, z < 3)):
            arrived(near_c.at[f, pl.ds(4 * n, 2)], near_sem.at[f, n], cond)
    for count, cond in ((5, (z == 0) | (z == 3)), (7, (z == 1) | (z == 2))):
        arrived(start.at[pl.ds(0, count), pl.ds(0, 112), :], state_sem, cond)

    first_low = 2 * z + 1

    def wrapped(ref, low, count):
        for k in range(count):
            ref[low + k, pl.ds(0, 8), :] = ref[low + k, pl.ds(128, 8), :]
            ref[low + k, pl.ds(136, 8), :] = ref[low + k, pl.ds(8, 8), :]

    wrapped(start, 2 * z, 8)

    def rows_of(i):
        def at(n, j):
            r = pl.ds(16 * i + 8 * j, 8)
            return near_c[1, n, r, :], near_c[0, n, r, :]

        return [8 + 16 * i, 16 + 16 * i], at

    def half_one(i, carry):
        starts, at = rows_of(i)
        planes = [(first_low + n, n, n) for n in range(6)]
        coarse_stage(start, mid, planes, starts, at)
        return carry

    lax.fori_loop(0, 8, half_one, 0, unroll=2)

    @pl.when(z == 0)
    def _():
        mid[pl.ds(0, 2)] = jnp.zeros((2, 144, 128), F32)

    @pl.when(z == 3)
    def _():
        mid[pl.ds(4, 2)] = jnp.zeros((2, 144, 128), F32)

    wrapped(mid, 0, 6)

    def half_two(i, carry):
        starts, at = rows_of(i)
        planes = [(n + 1, n, n + 1) for n in range(4)]
        coarse_stage(mid, end_state, planes, starts, at)
        return carry

    lax.fori_loop(0, 8, half_two, 0, unroll=2)
    states[0] = start[pl.ds(2 * z + 2, 4), pl.ds(8, 128), :]
    states[1] = mid[pl.ds(1, 4), pl.ds(8, 128), :] - warm[...]
    states[2] = end_state[:, pl.ds(8, 128), :] - warm[...]

    for low, index, cond in ((6, 1, z < 3), (0, 2, z > 0)):
        for piece in range(4):
            view = restart.at[pl.ds(low, 2), pl.ds(4 * piece, 4), c]
            arrived(view, halo_piece.at[index - 1, piece], cond)
        view = restart.at[pl.ds(low, 2), :, c]
        send(view, view, restart_sem.at[index + 2], partner, cond)
    for low, index, cond in ((6, 3, z < 3), (0, 4, z > 0)):
        arrived(restart.at[pl.ds(low, 2), :, 1 - c], restart_sem.at[index], cond)
    arrived(restart.at[pl.ds(2, 4), :, 1 - c], restart_sem.at[0])
    for index, view in enumerate((source_lo, source_hi, rate_lo, rate_hi)):
        arrived(view, halo_sem.at[index + 2], (z > 0) if index % 2 == 0 else (z < 3))
    for cond, wait in waits:
        guarded(cond, wait)


def fine_kernel(*refs):
    inputs, out = refs[:11], refs[11]
    half, lifted, mixed, base, extra, last, later = refs[12:19]
    held, load_sem = refs[19:30], refs[30]
    loads = [
        pltpu.make_async_copy(a, b, load_sem.at[n]) for n, (a, b) in enumerate(zip(inputs, held))
    ]
    for n in (10, 9, 0, 1, 2, 3, 4, 5, 6, 7, 8):
        loads[n].start()
    prev, prev_lo, prev_hi, source, source_lo, source_hi, rate, rate_lo, rate_hi, restart, states = held
    z = lax.axis_index("space")
    w = stencil_weights(1.0)
    pair = pair_table(256, 128)
    spread = (
        lax.broadcasted_iota(jnp.int32, (128, 256), 0)
        == lax.broadcasted_iota(jnp.int32, (128, 256), 1) // 2
    ).astype(F32)

    def prev_layer(k):
        return prev_lo.at[k] if k < 2 else prev_hi.at[k - 6] if k > 5 else prev.at[k - 2]

    def of(low, middle, high, k):
        return low.at[0] if k < 2 else high.at[0] if k > 5 else middle.at[k - 2]

    def inside(k):
        return (z > 0) if k < 2 else (z < 3) if k > 5 else None

    def masked(k, value):
        cond = inside(k)
        return value if cond is None else jnp.where(cond, value, 0.0)

    loads[10].wait()
    loads[9].wait()
    for k in range(4):
        seed_c = 0.125 * pooled(restart[2 * k] + restart[2 * k + 1], pair, half)
        for n in range(3):
            change = states[n, k] if n else states[n, k] - seed_c
            wide = jnp.dot(
                change, spread, precision=lax.Precision.HIGHEST, preferred_element_type=F32
            )
            for h in range(2):
                column = wide[:, 128 * h : 128 * h + 128]
                lifted[n, k, h, pl.ds(0, 128, stride=2), :] = column
                lifted[n, k, h, pl.ds(1, 128, stride=2), :] = column

    def share(v):
        return v * pl.reciprocal(1.0 + v * v)

    def put(ref, k, i, value):
        for h in range(2):
            ref[k, h, pl.ds(8 + 8 * i, 8), :] = value[:, 128 * h : 128 * h + 128]

    def row(ref, k, start):
        return jnp.concatenate([ref[k, h, pl.ds(start, 8), :] for h in range(2)], axis=-1)

    def guesses(i, carry):
        r = pl.ds(8 * i, 8)
        for k in range(8):
            lift = [
                jnp.concatenate([lifted[n, k // 2, h, r, :] for h in range(2)], axis=-1)
                for n in range(3)
            ]
            warm = prev_layer(k)[r, :]
            g = [masked(k, v) for v in (restart[k, r, :] + lift[0], warm + lift[1], warm + lift[2])]
            put(mixed, k, i, weights_one[0] * g[0] + weights_one[1] * g[1] + weights_one[2] * g[2])
            if 1 <= k <= 6:
                s = [share(v) for v in g]
                c = of(rate_lo, rate, rate_hi, k)[r, :]
                q = 0.5 * of(source_lo, source, source_hi, k)[r, :]
                base[k - 1, r, :] = (
                    g[0]
                    + c * (weights_one[0] * s[0] + weights_one[1] * s[1] + weights_one[2] * s[2])
                    + q
                )
                extra[k - 1, r, :] = (
                    weights_two[0] * g[0] + (weights_two[1] - 0.5) * g[1] + weights_two[2] * g[2]
                )
                if 2 <= k <= 5:
                    last[k - 2, r, :] = q + c * (
                        weights_two[0] * s[0]
                        + (weights_two[1] - 0.5) * s[1]
                        + weights_two[2] * s[2]
                    )
        return carry

    def wrap(ref, count):
        for k in range(count):
            for h in range(2):
                ref[k, h, pl.ds(0, 8), :] = ref[k, h, pl.ds(256, 8), :]
                ref[k, h, pl.ds(264, 8), :] = ref[k, h, pl.ds(8, 8), :]

    def linear(ref, k, i, below, here, above):
        r = 8 * i + 8
        value = w[0] * here + w[1] * above + w[2] * below
        value += w[3] * row(ref, k, r + 1) + w[4] * row(ref, k, r - 1)
        return value + w[5] * pltpu.roll(here, 255, 1) + w[6] * pltpu.roll(here, 1, 1)

    for n in range(9):
        loads[n].wait()
    lax.fori_loop(0, 32, guesses, 0, unroll=2)
    wrap(mixed, 8)

    def node_one(i, carry):
        r = pl.ds(8 * i, 8)
        planes = [row(mixed, k, 8 + 8 * i) for k in range(8)]
        for k in range(6):
            value = base[k, r, :] + linear(mixed, k + 1, i, *planes[k : k + 3])
            value = masked(0, value) if k == 0 else masked(7, value) if k == 5 else value
            if 1 <= k <= 4:
                out[0, 0, k - 1, r, :] = value
            put(later, k, i, 0.5 * value + extra[k, r, :])
        return carry

    lax.fori_loop(0, 32, node_one, 0, unroll=4)
    wrap(later, 6)

    def node_two(i, carry):
        r = pl.ds(8 * i, 8)
        planes = [row(later, k, 8 + 8 * i) for k in range(6)]
        for k in range(4):
            one = out[0, 0, k, r, :]
            value = one + 0.5 * rate[k, r, :] * share(one) + last[k, r, :]
            out[0, 1, k, r, :] = value + linear(later, k + 1, i, *planes[k : k + 3])
        return carry

    lax.fori_loop(0, 32, node_two, 0, unroll=4)


def shards(previous_end, source, rate):
    prev = previous_end[0]
    own = source[0]
    any_space = pl.BlockSpec(memory_space=pl.ANY)
    vmem = pl.BlockSpec(memory_space=pltpu.VMEM)
    dma = pltpu.SemaphoreType.DMA

    def shape(*dims):
        return jax.ShapeDtypeStruct(dims, F32)

    def scratch(*dims):
        return pltpu.VMEM(dims, F32)

    states, restart, *halos = pl.pallas_call(
        chain_kernel,
        out_shape=[shape(3, 4, 128, 128), shape(8, 16, 2, 8, 256)]
        + [shape(2, 256, 256)] * 2
        + [shape(1, 256, 256)] * 4,
        in_specs=[any_space] * 3,
        out_specs=[vmem] + [any_space] * 7,
        scratch_shapes=[
            scratch(4, 256, 256), scratch(4, 256, 256), scratch(4, 256, 256), scratch(256, 128),
            scratch(3, 2, 160, 128), scratch(32, 8, 64, 128), scratch(8, 48, 128),
            scratch(8, 48, 128), scratch(10, 64, 128), scratch(10, 64, 128),
            scratch(3, 8, 16, 128), scratch(3, 2, 8, 16, 128), scratch(2, 8, 16, 128),
            scratch(160, 128), scratch(14, 144, 128), scratch(6, 144, 128), scratch(4, 144, 128),
            scratch(2, 6, 128, 128), scratch(4, 128, 128),
            dma((3,)), dma((N_SEND,)), dma((32,)), dma((32,)), dma((2,)), dma, dma((3, 2)), dma,
            dma((6,)), dma((5,)), dma((2, 2)), dma((2, 4)),
        ],
        compiler_params=pltpu.CompilerParams(
            collective_id=0, has_side_effects=True, vmem_limit_bytes=63 * 1024 * 1024
        ),
    )(prev, own, rate)
    prev_lo, prev_hi, source_lo, source_hi, rate_lo, rate_hi = halos
    restart = restart.reshape(8, 256, 256)
    return pl.pallas_call(
        fine_kernel,
        out_shape=shape(1, 2, 4, 256, 256),
        in_specs=[any_space] * 11,
        out_specs=vmem,
        scratch_shapes=[
            scratch(256, 128), scratch(3, 4, 2, 256, 128), scratch(8, 2, 272, 128),
            scratch(6, 256, 256), scratch(6, 256, 256), scratch(4, 256, 256),
            scratch(6, 2, 272, 128),
            scratch(4, 256, 256), scratch(2, 256, 256), scratch(2, 256, 256),
            scratch(4, 256, 256), scratch(1, 256, 256), scratch(1, 256, 256),
            scratch(4, 256, 256), scratch(1, 256, 256), scratch(1, 256, 256),
            scratch(8, 256, 256), scratch(3, 4, 128, 128), dma((11,)),
        ],
        compiler_params=pltpu.CompilerParams(vmem_limit_bytes=63 * 1024 * 1024),
    )(prev, prev_lo, prev_hi, own, source_lo, source_hi, rate, rate_lo, rate_hi, restart, states)


def solution(mesh):
    torus = Mesh(
        mesh.devices.reshape(4, 4, 2, mesh.shape["space"]), ("tm_0", "tm_1", "tm_2", "space")
    )
    placed = (P(TM, "space", None, None), P(TM, "space", None, None), P("space", None, None))
    return jax.shard_map(
        shards,
        mesh=torus,
        in_specs=placed,
        out_specs=P(TM, None, "space", None, None),
        check_vma=False,
    )
```

```python
import jax
import jax.numpy as jnp
from jax import lax
from jax.experimental import pallas as pl
from jax.experimental.pallas import tpu as pltpu
from jax.sharding import Mesh
from jax.sharding import PartitionSpec as P

TM = ("tm_0", "tm_1", "tm_2")
AXES = TM + ("space",)
MESH = pl.DeviceIdType.MESH
F32 = jnp.float32

diffusion = 0.1
speed_z = 0.4
speed_x = 0.3
speed_y = 0.2
weights_one = (5.0 / 24.0, 1.0 / 3.0, -1.0 / 24.0)
weights_two = (-1.0 / 24.0, 1.0 / 3.0, 5.0 / 24.0)


def stencil_weights(spacing):
    d = diffusion / (spacing * spacing)
    out = [-6.0 * d]
    for speed in (speed_z, speed_x, speed_y):
        out += [d - speed / (2.0 * spacing), d + speed / (2.0 * spacing)]
    return out


def pair_table(fine, coarse):
    rows = lax.broadcasted_iota(jnp.int32, (fine, coarse), 0) // 2
    columns = lax.broadcasted_iota(jnp.int32, (fine, coarse), 1)
    return (rows == columns).astype(F32).astype(jnp.bfloat16)


def table_dot(value, table):
    out = None
    for _ in range(3):
        part = value.astype(jnp.bfloat16)
        value = value - part.astype(F32)
        term = jnp.dot(part, table, preferred_element_type=F32)
        out = term if out is None else out + term
    return out


def pooled(total, pair, scratch):
    scratch[...] = table_dot(total, pair)
    return scratch[pl.ds(0, 128, stride=2), :] + scratch[pl.ds(1, 128, stride=2), :]


def coarse_stage(src, dst, planes, starts, at):
    w = [0.5 * v for v in stencil_weights(2.0)]
    for j, r in enumerate(starts):
        below = src[planes[0][0] - 1, pl.ds(r, 8), :]
        here = src[planes[0][0], pl.ds(r, 8), :]
        for k, to, n in planes:
            above = src[k + 1, pl.ds(r, 8), :]
            rate, source = at(n, j)
            out = (1.0 + w[0]) * here + source
            out += w[1] * above + w[2] * below
            out += w[3] * src[k, pl.ds(r + 1, 8), :] + w[4] * src[k, pl.ds(r - 1, 8), :]
            out += w[5] * pltpu.roll(here, 127, 1) + w[6] * pltpu.roll(here, 1, 1)
            out += rate * here * pl.reciprocal(1.0 + here * here)
            dst[to, pl.ds(r, 8), :] = out
            below, here = here, above


N_SEND = 320


def chain_kernel(
    prev, source, rate,
    states, restart, prev_lo, prev_hi, source_lo, source_hi, rate_lo, rate_hi,
    fine_s, fine_r, fine_p, half, own, buf, rate_c, seed, state_a, state_b,
    edge_out, edge_in, found, layer, start, mid, end_state, near_c, warm,
    load_sem, send_sem, slot_sem, fine_sem, seed_sem, rate_sem, edge_sem, state_sem, halo_sem,
    restart_sem, near_sem, rate_half_sem,
):
    y, x, c, z = (lax.axis_index(name) for name in AXES)
    chip = y * 4 + x
    mine = chip * 2 + c
    slab = 2 * z + c
    is_last = mine == 31
    partner = (y, x, 1 - c, z)
    waits = []

    def guarded(cond, action):
        if cond is None:
            action()
        else:
            pl.when(cond)(action)

    def send(src, dst, sem, device, cond=None):
        index = len(waits)

        def build():
            return pltpu.make_async_remote_copy(
                src_ref=src, dst_ref=dst, send_sem=send_sem.at[index], recv_sem=sem,
                device_id=device, device_id_type=MESH,
            )

        waits.append((cond, lambda: build().wait_send()))
        guarded(cond, lambda: build().start())

    def arrived(view, sem, cond=None):
        def wait():
            pltpu.make_async_remote_copy(
                src_ref=view, dst_ref=view, send_sem=send_sem.at[0], recv_sem=sem,
                device_id=partner, device_id_type=MESH,
            ).wait_recv()

        guarded(cond, wait)

    def turned(value):
        return lax.rem(value + 8, 4)

    def first(step):
        return (turned(y + step * c), turned(x + step * (1 - c)), c, z)

    def second(step):
        return (turned(y + step * (1 - c)), turned(x + step * c), c, z)

    def slot(da, db):
        return (turned(y + da * c + db * (1 - c)) * 4 + turned(x + da * (1 - c) + db * c)) * 2 + c

    load_p = pltpu.make_async_copy(prev, fine_p, load_sem.at[0])
    load_s = pltpu.make_async_copy(source, fine_s, load_sem.at[1])
    load_r = pltpu.make_async_copy(rate, fine_r, load_sem.at[2])
    load_p.start()
    load_s.start()
    load_r.start()
    barrier = pltpu.get_barrier_semaphore()
    plane = [(dy, dx) for dy in range(4) for dx in range(4) if dy or dx]
    peers = [(turned(y + dy), turned(x + dx), c, z) for dy, dx in plane]
    peers += [(y, x, c, turned(z + d)) for d in (1, 2, 3)]
    peers += [(y, x, 1 - c, turned(z + d)) for d in (0, 1, 2, 3)]
    for device in peers:
        pl.semaphore_signal(barrier, inc=1, device_id=device, device_id_type=MESH)

    def greet(step):
        to = (3, 3, 1, turned(z + step))
        pl.semaphore_signal(barrier, inc=1, device_id=to, device_id_type=MESH)

    pl.when(jnp.logical_not(is_last))(lambda: greet(0))
    pl.when(z > 0)(lambda: greet(-1))
    pl.when(z < 3)(lambda: greet(1))
    inner_z = (z > 0) & (z < 3)
    more = jnp.where(is_last, jnp.where(inner_z, 95, 63), 0)

    pair = pair_table(256, 128)

    def restrict(fine, index, scale):
        for k in range(2):
            total = scale * pooled(fine[2 * k] + fine[2 * k + 1], pair, half)
            own[index, k, pl.ds(16, 128), :] = total
            own[index, k, pl.ds(0, 16), :] = total[112:128]
            own[index, k, pl.ds(144, 16), :] = total[0:16]

    load_p.wait()
    pl.when(is_last)(lambda: restrict(fine_p, 2, 0.125))
    load_s.wait()
    restrict(fine_s, 0, 0.0625)
    pl.semaphore_wait(barrier, len(peers) + more)

    layers = pl.ds(2 * z, 2)
    rows = pl.ds(16 * c, 48)
    along = x * (1 - c) + y * c
    across = y * (1 - c) + x * c
    in_line = across == 3
    is_root = in_line & (along == 3)

    send(own.at[2, 1], layer, seed_sem.at[0], partner, is_last)

    def seed_self():
        layer[...] = own[2, 0]

    pl.when(is_last)(seed_self)

    for d in (1, 3, 2):
        to = turned(z + d)
        send(
            own.at[0, :, pl.ds(32 * to, 64), :], buf.at[mine, layers], slot_sem.at[mine],
            (y, x, c, to),
        )
    buf[mine, layers] = own[0, :, pl.ds(32 * z, 64), :]
    arrived(layer, seed_sem.at[0], mine == 30)
    for d in (2, 1, -1):
        send(layer, layer, seed_sem.at[0], first(d), is_root)

    def fine_halo(field, low, high, width, index):
        send(
            field.at[pl.ds(4 - width, width)], low, halo_sem.at[index], (y, x, c, turned(z + 1)),
            z < 3,
        )
        send(
            field.at[pl.ds(0, width)], high, halo_sem.at[index + 1], (y, x, c, turned(z - 1)),
            z > 0,
        )

    def along_z(pieces, sems, index):
        for (src, dst), n, step, cond in zip(pieces, (0, 1), (1, -1), (z < 3, z > 0)):
            send(src, dst, sems.at[index, n], (y, x, c, turned(z + step)), cond)

    def other_halos():
        src = own.at[0, :, pl.ds(16, 128), :]
        along_z([(src, near_c.at[0, pl.ds(4 * n, 2)]) for n in range(2)], near_sem, 0)
        fine_halo(source, source_lo, source_hi, 1, 2)

    rate_rows = pl.ds(128 * c, 128)
    rate_views = [view.at[:, rate_rows, :] for view in (rate_lo, rate_hi)]
    rate_c_views = [near_c.at[1, pl.ds(4 * n + c, 1)] for n in range(2)]
    rate_others = [view.at[:, pl.ds(128 * (1 - c), 128), :] for view in (rate_lo, rate_hi)]
    rate_c_others = [near_c.at[1, pl.ds(4 * n + 1 - c, 1)] for n in range(2)]

    def rate_fine():
        srcs = [rate.at[pl.ds(3 * (1 - n), 1), rate_rows, :] for n in range(2)]
        along_z(zip(srcs, rate_views), rate_half_sem, 0)

    def rate_coarse():
        src = own.at[1, pl.ds(c, 1), pl.ds(16, 128), :]
        along_z([(src, view) for view in rate_c_views], near_sem, 1)

    def rate_across():
        for views, sems, index in ((rate_c_views, near_sem, 1), (rate_views, rate_half_sem, 0)):
            for n, cond in ((0, z > 0), (1, z < 3)):
                arrived(views[n], sems.at[index, n], cond)
                send(views[n], views[n], rate_half_sem.at[1 + index, n], partner, cond)

    fine_halo(prev, prev_lo, prev_hi, 2, 0)

    def fine_own():
        for n in range(30, -1, -1):
            send(
                fine_p.at[:, pl.ds(8 * n, 8), :], restart.at[pl.ds(2, 4), n // 2, n % 2],
                fine_sem.at[0, n], (n // 8, n // 2 % 4, n % 2, z), is_last,
            )

        @pl.when(is_last)
        def _():
            local = pltpu.make_async_copy(
                fine_p.at[:, pl.ds(248, 8), :], restart.at[pl.ds(2, 4), 15, 1], load_sem.at[0]
            )
            local.start()
            local.wait()

    def fine_beside():
        for n in range(31, -1, -1):
            for low, to, step, index, cond in (
                (2, 0, 1, 1, is_last & (z < 3)),
                (0, 6, -1, 2, is_last & (z > 0)),
            ):
                send(
                    fine_p.at[pl.ds(low, 2), pl.ds(8 * n, 8), :],
                    restart.at[pl.ds(to, 2), n // 2, n % 2], fine_sem.at[index, n],
                    (n // 8, n // 2 % 4, n % 2, turned(z + step)), cond,
                )

    fine_parts = (
        (0, 2, 4, jnp.logical_not(is_last), None), (1, 0, 2, z > 0, z > 0), (2, 6, 2, z < 3, z < 3)
    )

    def fine_direct(index):
        _, low, count, ready_cond, cond = fine_parts[index]
        view = restart.at[pl.ds(low, count), chip, c]
        arrived(view, fine_sem.at[index, mine], ready_cond)
        for dy, dx in plane:
            to = (turned(y + dy), turned(x + dx), c, z)
            send(view, view, fine_sem.at[index, mine], to, cond)

    def fine_across():
        for index, low, count, _, cond in fine_parts:
            for dy, dx in plane:
                other = turned(y + dy) * 4 + turned(x + dx)
                view = restart.at[pl.ds(low, count), other, c]
                arrived(view, fine_sem.at[index, other * 2 + c], cond)
            view = restart.at[pl.ds(low, count), :, c]
            send(view, view, restart_sem.at[index], partner, cond)

    def fine_ready():
        for index, low, count, _, cond in fine_parts:
            arrived(restart.at[pl.ds(low, count), :, 1 - c], restart_sem.at[index], cond)

    fine_own()
    load_r.wait()
    restrict(fine_r, 1, 0.0625)
    for d in (1, 3, 2):
        to = turned(z + d)
        send(
            own.at[1, :, pl.ds(32 * to + 16 * c, 48), :], rate_c.at[layers], rate_sem,
            (y, x, c, to),
        )
    rate_c[layers] = own[1, :, pl.ds(32 * z + 16 * c, 48), :]
    arrived(layer, seed_sem.at[0], in_line & (along != 3))
    for d in (2, 1, -1):
        send(layer, layer, seed_sem.at[0], second(d), in_line)

    def spread_seed():
        arrived(layer, seed_sem.at[0], jnp.logical_not(in_line))
        target = 2 * z + 1 - c
        for d in (1, 3, 2, 0):
            for core in (0, 1):
                to = turned(z + d)
                view = layer.at[pl.ds(32 * to + 16 * core, 48), :]
                cond = None if d else (c != core)
                send(view, seed.at[target], seed_sem.at[1], (y, x, core, to), cond)
        seed[target] = layer[pl.ds(32 * z + 16 * c, 48), :]

    def chunk(da, db):
        return buf.at[slot(da, db)], slot_sem.at[slot(da, db)]

    def across_chip(da, db, cond=None):
        view = buf.at[slot(da, db), :, pl.ds(16 * (1 - c), 48), :]
        send(view, view, slot_sem.at[slot(da, db)], partner, cond)

    def onward(da, db):
        full, sem = chunk(da, db)
        for step in (1, -1):
            send(full, full, sem, second(step))
        across_chip(da, db)

    def relay(da, db, device, h):
        full, sem = chunk(da, db)
        arrived(full, sem)
        view = buf.at[slot(da, db), pl.ds(4 * h, 4)]
        send(view, view, sem, device)

    def near(relay, onward):
        relay(-1, 0, first(1), 0)
        onward(-1, 0)
        relay(1, 0, first(-1), 1)
        onward(1, 0)

    def ring(relay, a):
        for step, h in ((-1, 0), (1, 1)):
            relay(a, step, second(-step), h)
            across_chip(a, step)

    full, sem = chunk(0, 0)
    arrived(full.at[pl.ds(0, 6)], sem)
    for step in (1, -1):
        send(full, full, sem, first(step))
    onward(0, 0)
    near(relay, onward)
    spread_seed()
    other_halos()
    ring(relay, 0)
    arrived(*chunk(2, 0))
    onward(2, 0)
    ring(relay, -1)
    ring(relay, 1)
    arrived(*chunk(0, 2))
    across_chip(0, 2)
    ring(relay, 2)
    fine_beside()

    def ready(block):
        for a in (-1, 1, 2):
            here = slot(a, 2)
            cond = here // 8 == block
            arrived(*chunk(a, 2), cond)
            across_chip(a, 2, cond)
        for b in range(4):
            other = (block * 4 + b) * 2 + 1 - c
            arrived(buf.at[other, :, rows, :], slot_sem.at[other])

    arrived(rate_c.at[pl.ds(0, 6)], rate_sem)
    arrived(seed.at[pl.ds(0, 7)], seed_sem.at[1])

    state_a[...] = jnp.zeros_like(state_a)
    state_b[...] = jnp.zeros_like(state_b)
    state_a[pl.ds(1, 8), pl.ds(8, 48), :] = seed[...]
    inner = pl.ds(24, 16)
    up = (y, x, 1 - c, turned(z + c))
    down = (y, x, 1 - c, turned(z - 1 + c))

    def run(block, low, count, tiles):
        def body(i, carry):
            t = block * 8 + low + i

            @pl.when(t == 2 * chip)
            def _():
                found[0] = state_a[pl.ds(1, 8), inner, :]

            def at(n, j):
                r = 8 * tiles[j]
                return rate_c[n, pl.ds(r, 8), :], buf[t, n, pl.ds(16 * c + r, 8), :]

            planes = [(k, k, k - 1) for k in range(1, 9)]
            starts = [8 + 8 * tile for tile in tiles]
            coarse_stage(state_a, state_b, planes, starts, at)
            coarse_stage(state_b, state_a, planes, starts, at)
            return carry

        lax.fori_loop(0, count, body, 0)

    for block in range(4):
        active = y >= block
        if block:
            e = block - 1

            def fill(e=e):
                edge_out[e] = state_a[pl.ds(1, 8), inner, :]

            pl.when(active)(fill)
            send(edge_out.at[e], edge_in.at[e, 0], edge_sem.at[e, 0], up, active)
            send(edge_out.at[e], edge_in.at[e, 1], edge_sem.at[e, 1], down, active)
            if block == 1:
                rate_fine()
                fine_direct(0)
            if block == 2:
                rate_coarse()
                fine_direct(1)
                fine_direct(2)
            arrived(edge_in.at[e, 0], edge_sem.at[e, 0], active)
            arrived(edge_in.at[e, 1], edge_sem.at[e, 1], active)

            def spill(e=e):
                state_a[pl.ds(1, 8), pl.ds(8, 16), :] = edge_in[e, 0]
                state_a[pl.ds(1, 8), pl.ds(40, 16), :] = edge_in[e, 1]

            pl.when(active)(spill)
        ready(block)
        count = jnp.where(y > block, 8, jnp.where(active, 2 * x + 1, 0))
        run(block, 0, jnp.minimum(count, 4), range(6))
        run(block, 4, jnp.maximum(count - 4, 0), range(1, 5))

    found[1] = state_a[pl.ds(1, 8), inner, :]
    here = pl.ds(8 + 16 * slab, 16)
    for d in (1, 3, 2, 0):
        to = turned(z + d)
        end = (to == 0) | (to == 3)
        for core in (0, 1):
            for count, low, cond in (
                (5, jnp.where(to == 0, 0, 3), end),
                (7, jnp.where(to == 1, 0, 1), jnp.logical_not(end)),
            ):
                send(
                    found.at[core, pl.ds(low, count)], start.at[pl.ds(3 + low, count), here, :],
                    state_sem, (y, x, core, to), cond if d else cond & (c != core),
                )
    rate_across()
    zero = jnp.zeros((3, 144, 128), F32)
    start[pl.ds(0, 3)] = zero
    start[pl.ds(11, 3)] = zero
    start[pl.ds(3, 8), here, :] = found[c]

    for index in (0, 1):
        arrived((prev_lo, prev_hi)[index], halo_sem.at[index], (z < 3) if index else (z > 0))
    sides = [
        pltpu.make_async_copy(view, fine_r.at[pl.ds(2 * n, 2)], load_sem.at[1 + n])
        for n, view in enumerate((prev_lo, prev_hi))
    ]
    for copy in sides:
        copy.start()
    for n in range(2):
        warm[1 + n] = 0.125 * pooled(fine_p[2 * n] + fine_p[2 * n + 1], pair, half)
    for copy in sides:
        copy.wait()
    for n in range(2):
        warm[3 * n] = 0.125 * pooled(fine_r[2 * n] + fine_r[2 * n + 1], pair, half)
    for f in range(2):
        near_c[f, pl.ds(2, 2)] = own[f, :, pl.ds(16, 128), :]
    for n, cond in ((0, z > 0), (1, z < 3)):
        arrived(near_c.at[0, pl.ds(4 * n, 2)], near_sem.at[0, n], cond)
        arrived(rate_c_others[n], rate_half_sem.at[2, n], cond)
    fine_across()
    for count, cond in ((5, (z == 0) | (z == 3)), (7, (z == 1) | (z == 2))):
        arrived(start.at[pl.ds(0, count), pl.ds(0, 112), :], state_sem, cond)

    first_low = 2 * z + 1

    def wrapped(ref, low, count):
        for k in range(count):
            ref[low + k, pl.ds(0, 8), :] = ref[low + k, pl.ds(128, 8), :]
            ref[low + k, pl.ds(136, 8), :] = ref[low + k, pl.ds(8, 8), :]

    wrapped(start, 2 * z, 8)

    def rows_of(i):
        def at(n, j):
            r = pl.ds(16 * i + 8 * j, 8)
            return near_c[1, n, r, :], near_c[0, n, r, :]

        return [8 + 16 * i, 16 + 16 * i], at

    def half_one(i, carry):
        starts, at = rows_of(i)
        planes = [(first_low + n, n, n) for n in range(6)]
        coarse_stage(start, mid, planes, starts, at)
        return carry

    lax.fori_loop(0, 8, half_one, 0, unroll=2)

    @pl.when(z == 0)
    def _():
        mid[pl.ds(0, 2)] = jnp.zeros((2, 144, 128), F32)

    @pl.when(z == 3)
    def _():
        mid[pl.ds(4, 2)] = jnp.zeros((2, 144, 128), F32)

    wrapped(mid, 0, 6)

    def half_two(i, carry):
        starts, at = rows_of(i)
        planes = [(n + 1, n, n + 1) for n in range(4)]
        coarse_stage(mid, end_state, planes, starts, at)
        return carry

    lax.fori_loop(0, 8, half_two, 0, unroll=2)
    states[0] = start[pl.ds(2 * z + 2, 4), pl.ds(8, 128), :]
    states[1] = mid[pl.ds(1, 4), pl.ds(8, 128), :] - warm[...]
    states[2] = end_state[:, pl.ds(8, 128), :] - warm[...]

    fine_ready()
    for n, cond in ((0, z > 0), (1, z < 3)):
        arrived((source_lo, source_hi)[n], halo_sem.at[2 + n], cond)
        arrived(rate_others[n], rate_half_sem.at[1, n], cond)
    assert len(waits) <= N_SEND
    for cond, wait in waits:
        guarded(cond, wait)


def fine_kernel(*refs):
    inputs, result = refs[:11], refs[11]
    half, lifted, mixed, base, extra, last, later = refs[12:19]
    held, load_sem = refs[19:30], refs[30]
    out, store_sem = refs[31], refs[32]
    loads = [
        pltpu.make_async_copy(a, b, load_sem.at[n]) for n, (a, b) in enumerate(zip(inputs, held))
    ]
    for n in (10, 9, 0, 1, 2, 3, 4, 5, 6, 7, 8):
        loads[n].start()
    prev, prev_lo, prev_hi, source, source_lo, source_hi, rate, rate_lo, rate_hi, restart, states = held
    z = lax.axis_index("space")
    w = stencil_weights(1.0)
    pair = pair_table(256, 128)
    spread = (
        lax.broadcasted_iota(jnp.int32, (128, 256), 0)
        == lax.broadcasted_iota(jnp.int32, (128, 256), 1) // 2
    ).astype(F32).astype(jnp.bfloat16)

    def prev_layer(k):
        return prev_lo.at[k] if k < 2 else prev_hi.at[k - 6] if k > 5 else prev.at[k - 2]

    def of(low, middle, high, k):
        return low.at[0] if k < 2 else high.at[0] if k > 5 else middle.at[k - 2]

    def inside(k):
        return (z > 0) if k < 2 else (z < 3) if k > 5 else None

    def masked(k, value):
        cond = inside(k)
        return value if cond is None else jnp.where(cond, value, 0.0)

    loads[10].wait()

    def lift(n, change):
        wide = table_dot(change.reshape(512, 128), spread)
        for k in range(4):
            for h in range(2):
                column = wide[128 * k : 128 * k + 128, 128 * h : 128 * h + 128]
                lifted[n, k, h, pl.ds(0, 128, stride=2), :] = column
                lifted[n, k, h, pl.ds(1, 128, stride=2), :] = column

    lift(1, states[1])
    lift(2, states[2])
    loads[9].wait()
    for k in range(4):
        seed_c = 0.125 * pooled(restart[2 * k] + restart[2 * k + 1], pair, half)
        states[0, k] = states[0, k] - seed_c
    lift(0, states[0])

    def share(v):
        return v * pl.reciprocal(1.0 + v * v)

    def put(ref, k, i, value):
        for h in range(2):
            ref[k, h, pl.ds(8 + 8 * i, 8), :] = value[:, 128 * h : 128 * h + 128]

    def row(ref, k, start):
        return jnp.concatenate([ref[k, h, pl.ds(start, 8), :] for h in range(2)], axis=-1)

    def guesses(i, carry):
        r = pl.ds(8 * i, 8)
        for k in range(8):
            lift = [
                jnp.concatenate([lifted[n, k // 2, h, r, :] for h in range(2)], axis=-1)
                for n in range(3)
            ]
            warm = prev_layer(k)[r, :]
            g = [masked(k, v) for v in (restart[k, r, :] + lift[0], warm + lift[1], warm + lift[2])]
            put(mixed, k, i, weights_one[0] * g[0] + weights_one[1] * g[1] + weights_one[2] * g[2])
            if 1 <= k <= 6:
                s = [share(v) for v in g]
                c = of(rate_lo, rate, rate_hi, k)[r, :]
                q = 0.5 * of(source_lo, source, source_hi, k)[r, :]
                base[k - 1, r, :] = (
                    g[0]
                    + c * (weights_one[0] * s[0] + weights_one[1] * s[1] + weights_one[2] * s[2])
                    + q
                )
                extra[k - 1, r, :] = (
                    weights_two[0] * g[0] + (weights_two[1] - 0.5) * g[1] + weights_two[2] * g[2]
                )
                if 2 <= k <= 5:
                    last[k - 2, r, :] = q + c * (
                        weights_two[0] * s[0]
                        + (weights_two[1] - 0.5) * s[1]
                        + weights_two[2] * s[2]
                    )
        return carry

    def wrap(ref, count):
        for k in range(count):
            for h in range(2):
                ref[k, h, pl.ds(0, 8), :] = ref[k, h, pl.ds(256, 8), :]
                ref[k, h, pl.ds(264, 8), :] = ref[k, h, pl.ds(8, 8), :]

    def linear(ref, k, i, below, here, above):
        r = 8 * i + 8
        value = w[0] * here + w[1] * above + w[2] * below
        value += w[3] * row(ref, k, r + 1) + w[4] * row(ref, k, r - 1)
        return value + w[5] * pltpu.roll(here, 255, 1) + w[6] * pltpu.roll(here, 1, 1)

    for n in range(9):
        loads[n].wait()
    lax.fori_loop(0, 32, guesses, 0, unroll=2)
    wrap(mixed, 8)

    def node_one(i, carry):
        r = pl.ds(8 * i, 8)
        planes = [row(mixed, k, 8 + 8 * i) for k in range(8)]
        for k in range(6):
            value = base[k, r, :] + linear(mixed, k + 1, i, *planes[k : k + 3])
            value = masked(0, value) if k == 0 else masked(7, value) if k == 5 else value
            if 1 <= k <= 4:
                out[0, 0, k - 1, r, :] = value
            put(later, k, i, 0.5 * value + extra[k, r, :])
        return carry

    lax.fori_loop(0, 32, node_one, 0, unroll=4)
    wrap(later, 6)
    stores = [
        pltpu.make_async_copy(out.at[0, n], result.at[0, n], store_sem.at[n]) for n in range(2)
    ]
    stores[0].start()

    def node_two(i, carry):
        r = pl.ds(8 * i, 8)
        planes = [row(later, k, 8 + 8 * i) for k in range(6)]
        for k in range(4):
            one = out[0, 0, k, r, :]
            value = one + 0.5 * rate[k, r, :] * share(one) + last[k, r, :]
            out[0, 1, k, r, :] = value + linear(later, k + 1, i, *planes[k : k + 3])
        return carry

    lax.fori_loop(0, 32, node_two, 0, unroll=4)
    stores[1].start()
    for copy in stores:
        copy.wait()


def shards(previous_end, source, rate):
    prev = previous_end[0]
    own = source[0]
    any_space = pl.BlockSpec(memory_space=pl.ANY)
    vmem = pl.BlockSpec(memory_space=pltpu.VMEM)
    dma = pltpu.SemaphoreType.DMA

    def shape(*dims):
        return jax.ShapeDtypeStruct(dims, F32)

    def scratch(*dims):
        return pltpu.VMEM(dims, F32)

    states, restart, *halos = pl.pallas_call(
        chain_kernel,
        out_shape=[shape(3, 4, 128, 128), shape(8, 16, 2, 8, 256)]
        + [shape(2, 256, 256)] * 2
        + [shape(1, 256, 256)] * 4,
        in_specs=[any_space] * 3,
        out_specs=[vmem] + [any_space] * 7,
        scratch_shapes=[
            scratch(4, 256, 256), scratch(4, 256, 256), scratch(4, 256, 256), scratch(256, 128),
            scratch(3, 2, 160, 128), scratch(32, 8, 64, 128), scratch(8, 48, 128),
            scratch(8, 48, 128), scratch(10, 64, 128), scratch(10, 64, 128),
            scratch(3, 8, 16, 128), scratch(3, 2, 8, 16, 128), scratch(2, 8, 16, 128),
            scratch(160, 128), scratch(14, 144, 128), scratch(6, 144, 128), scratch(4, 144, 128),
            scratch(2, 6, 128, 128), scratch(4, 128, 128),
            dma((3,)), dma((N_SEND,)), dma((32,)), dma((3, 32)), dma((2,)), dma, dma((3, 2)), dma,
            dma((4,)), dma((3,)), dma((2, 2)), dma((3, 2)),
        ],
        compiler_params=pltpu.CompilerParams(
            collective_id=0, has_side_effects=True, vmem_limit_bytes=63 * 1024 * 1024
        ),
    )(prev, own, rate)
    prev_lo, prev_hi, source_lo, source_hi, rate_lo, rate_hi = halos
    restart = restart.reshape(8, 256, 256)
    return pl.pallas_call(
        fine_kernel,
        out_shape=shape(1, 2, 4, 256, 256),
        in_specs=[any_space] * 11,
        out_specs=any_space,
        scratch_shapes=[
            scratch(256, 128), scratch(3, 4, 2, 256, 128), scratch(8, 2, 272, 128),
            scratch(6, 256, 256), scratch(6, 256, 256), scratch(4, 256, 256),
            scratch(6, 2, 272, 128),
            scratch(4, 256, 256), scratch(2, 256, 256), scratch(2, 256, 256),
            scratch(4, 256, 256), scratch(1, 256, 256), scratch(1, 256, 256),
            scratch(4, 256, 256), scratch(1, 256, 256), scratch(1, 256, 256),
            scratch(8, 256, 256), scratch(3, 4, 128, 128), dma((11,)),
            scratch(1, 2, 4, 256, 256), dma((2,)),
        ],
        compiler_params=pltpu.CompilerParams(vmem_limit_bytes=63 * 1024 * 1024),
    )(prev, prev_lo, prev_hi, own, source_lo, source_hi, rate, rate_lo, rate_hi, restart, states)


def solution(mesh):
    torus = Mesh(
        mesh.devices.reshape(4, 4, 2, mesh.shape["space"]), ("tm_0", "tm_1", "tm_2", "space")
    )
    placed = (P(TM, "space", None, None), P(TM, "space", None, None), P("space", None, None))
    return jax.shard_map(
        shards,
        mesh=torus,
        in_specs=placed,
        out_specs=P(TM, None, "space", None, None),
        check_vma=False,
    )
```

```python
import jax
import jax.numpy as jnp
from jax import lax
from jax.experimental import pallas as pl
from jax.experimental.pallas import tpu as pltpu
from jax.sharding import Mesh
from jax.sharding import PartitionSpec as P

TM = ("tm_0", "tm_1", "tm_2")
AXES = TM + ("space",)
MESH = pl.DeviceIdType.MESH
F32 = jnp.float32

diffusion = 0.1
speed_z = 0.4
speed_x = 0.3
speed_y = 0.2
weights_one = (5.0 / 24.0, 1.0 / 3.0, -1.0 / 24.0)
weights_two = (-1.0 / 24.0, 1.0 / 3.0, 5.0 / 24.0)


def stencil_weights(spacing):
    d = diffusion / (spacing * spacing)
    out = [-6.0 * d]
    for speed in (speed_z, speed_x, speed_y):
        out += [d - speed / (2.0 * spacing), d + speed / (2.0 * spacing)]
    return out


def pair_table(fine, coarse):
    rows = lax.broadcasted_iota(jnp.int32, (fine, coarse), 0) // 2
    columns = lax.broadcasted_iota(jnp.int32, (fine, coarse), 1)
    return (rows == columns).astype(F32).astype(jnp.bfloat16)


def table_dot(value, table):
    out = None
    for _ in range(3):
        part = value.astype(jnp.bfloat16)
        value = value - part.astype(F32)
        term = jnp.dot(part, table, preferred_element_type=F32)
        out = term if out is None else out + term
    return out


def pooled(total, pair, scratch):
    scratch[...] = table_dot(total, pair)
    return scratch[pl.ds(0, 128, stride=2), :] + scratch[pl.ds(1, 128, stride=2), :]


def coarse_stage(src, dst, planes, starts, at):
    w = [0.5 * v for v in stencil_weights(2.0)]
    for j, r in enumerate(starts):
        below = src[planes[0][0] - 1, pl.ds(r, 8), :]
        here = src[planes[0][0], pl.ds(r, 8), :]
        for k, to, n in planes:
            above = src[k + 1, pl.ds(r, 8), :]
            rate, source = at(n, j)
            out = (1.0 + w[0]) * here + source
            out += w[1] * above + w[2] * below
            out += w[3] * src[k, pl.ds(r + 1, 8), :] + w[4] * src[k, pl.ds(r - 1, 8), :]
            out += w[5] * pltpu.roll(here, 127, 1) + w[6] * pltpu.roll(here, 1, 1)
            out += rate * here * pl.reciprocal(1.0 + here * here)
            dst[to, pl.ds(r, 8), :] = out
            below, here = here, above


N_SEND = 320


def chain_kernel(
    prev, source, rate,
    states, restart, prev_lo, prev_hi, source_lo, source_hi, rate_lo, rate_hi,
    fine_s, fine_r, fine_p, half, own, buf, rate_c, seed, state_a, state_b,
    edge_out, edge_in, found, layer, start, mid, end_state, near_c, warm,
    load_sem, send_sem, slot_sem, fine_sem, seed_sem, rate_sem, edge_sem, state_sem, halo_sem,
    restart_sem, near_sem, rate_half_sem,
):
    y, x, c, z = (lax.axis_index(name) for name in AXES)
    chip = y * 4 + x
    mine = chip * 2 + c
    slab = 2 * z + c
    is_last = mine == 31
    partner = (y, x, 1 - c, z)
    waits = []

    def guarded(cond, action):
        if cond is None:
            action()
        else:
            pl.when(cond)(action)

    def send(src, dst, sem, device, cond=None):
        index = len(waits)

        def build():
            return pltpu.make_async_remote_copy(
                src_ref=src, dst_ref=dst, send_sem=send_sem.at[index], recv_sem=sem,
                device_id=device, device_id_type=MESH,
            )

        waits.append((cond, lambda: build().wait_send()))
        guarded(cond, lambda: build().start())

    def arrived(view, sem, cond=None):
        def wait():
            pltpu.make_async_remote_copy(
                src_ref=view, dst_ref=view, send_sem=send_sem.at[0], recv_sem=sem,
                device_id=partner, device_id_type=MESH,
            ).wait_recv()

        guarded(cond, wait)

    def turned(value):
        return lax.rem(value + 8, 4)

    def first(step):
        return (turned(y + step * c), turned(x + step * (1 - c)), c, z)

    def second(step):
        return (turned(y + step * (1 - c)), turned(x + step * c), c, z)

    def slot(da, db):
        return (turned(y + da * c + db * (1 - c)) * 4 + turned(x + da * (1 - c) + db * c)) * 2 + c

    load_p = pltpu.make_async_copy(prev, fine_p, load_sem.at[0])
    load_s = pltpu.make_async_copy(source, fine_s, load_sem.at[1])
    load_r = pltpu.make_async_copy(rate, fine_r, load_sem.at[2])
    load_p.start()
    load_s.start()
    load_r.start()
    barrier = pltpu.get_barrier_semaphore()
    plane = [(dy, dx) for dy in range(4) for dx in range(4) if dy or dx]
    peers = [(turned(y + dy), turned(x + dx), c, z) for dy, dx in plane]
    peers += [(y, x, c, turned(z + d)) for d in (1, 2, 3)]
    peers += [(y, x, 1 - c, turned(z + d)) for d in (0, 1, 2, 3)]
    for device in peers:
        pl.semaphore_signal(barrier, inc=1, device_id=device, device_id_type=MESH)

    def greet(step):
        to = (3, 3, 1, turned(z + step))
        pl.semaphore_signal(barrier, inc=1, device_id=to, device_id_type=MESH)

    pl.when(jnp.logical_not(is_last))(lambda: greet(0))
    pl.when(z > 0)(lambda: greet(-1))
    pl.when(z < 3)(lambda: greet(1))
    inner_z = (z > 0) & (z < 3)
    more = jnp.where(is_last, jnp.where(inner_z, 95, 63), 0)

    pair = pair_table(256, 128)

    def restrict(fine, index, scale):
        for k in range(2):
            total = scale * pooled(fine[2 * k] + fine[2 * k + 1], pair, half)
            own[index, k, pl.ds(16, 128), :] = total
            own[index, k, pl.ds(0, 16), :] = total[112:128]
            own[index, k, pl.ds(144, 16), :] = total[0:16]

    load_p.wait()
    pl.when(is_last)(lambda: restrict(fine_p, 2, 0.125))
    load_s.wait()
    restrict(fine_s, 0, 0.0625)
    pl.semaphore_wait(barrier, len(peers) + more)

    layers = pl.ds(2 * z, 2)
    rows = pl.ds(16 * c, 48)
    along = x * (1 - c) + y * c
    across = y * (1 - c) + x * c
    in_line = across == 3
    is_root = in_line & (along == 3)

    send(own.at[2, 1], layer, seed_sem.at[0], partner, is_last)

    def seed_self():
        layer[...] = own[2, 0]

    pl.when(is_last)(seed_self)

    for d in (1, 3, 2):
        to = turned(z + d)
        send(
            own.at[0, :, pl.ds(32 * to, 64), :], buf.at[mine, layers], slot_sem.at[mine],
            (y, x, c, to),
        )
    buf[mine, layers] = own[0, :, pl.ds(32 * z, 64), :]
    arrived(layer, seed_sem.at[0], mine == 30)
    for d in (2, 1, -1):
        send(layer, layer, seed_sem.at[0], first(d), is_root)

    def fine_halo(field, low, high, width, index):
        send(
            field.at[pl.ds(4 - width, width)], low, halo_sem.at[index], (y, x, c, turned(z + 1)),
            z < 3,
        )
        send(
            field.at[pl.ds(0, width)], high, halo_sem.at[index + 1], (y, x, c, turned(z - 1)),
            z > 0,
        )

    def along_z(pieces, sems, index):
        for (src, dst), n, step, cond in zip(pieces, (0, 1), (1, -1), (z < 3, z > 0)):
            send(src, dst, sems.at[index, n], (y, x, c, turned(z + step)), cond)

    def other_halos():
        src = own.at[0, :, pl.ds(16, 128), :]
        along_z([(src, near_c.at[0, pl.ds(4 * n, 2)]) for n in range(2)], near_sem, 0)
        fine_halo(source, source_lo, source_hi, 1, 2)

    rate_rows = pl.ds(128 * c, 128)
    rate_views = [view.at[:, rate_rows, :] for view in (rate_lo, rate_hi)]
    rate_c_views = [near_c.at[1, pl.ds(4 * n + c, 1)] for n in range(2)]
    rate_others = [view.at[:, pl.ds(128 * (1 - c), 128), :] for view in (rate_lo, rate_hi)]
    rate_c_others = [near_c.at[1, pl.ds(4 * n + 1 - c, 1)] for n in range(2)]

    def rate_fine():
        srcs = [rate.at[pl.ds(3 * (1 - n), 1), rate_rows, :] for n in range(2)]
        along_z(zip(srcs, rate_views), rate_half_sem, 0)

    def rate_coarse():
        src = own.at[1, pl.ds(c, 1), pl.ds(16, 128), :]
        along_z([(src, view) for view in rate_c_views], near_sem, 1)

    def rate_across():
        for views, sems, index in ((rate_c_views, near_sem, 1), (rate_views, rate_half_sem, 0)):
            for n, cond in ((0, z > 0), (1, z < 3)):
                arrived(views[n], sems.at[index, n], cond)
                send(views[n], views[n], rate_half_sem.at[1 + index, n], partner, cond)

    fine_halo(prev, prev_lo, prev_hi, 2, 0)

    def fine_own():
        for n in range(30, -1, -1):
            send(
                fine_p.at[:, pl.ds(8 * n, 8), :], restart.at[pl.ds(2, 4), n // 2, n % 2],
                fine_sem.at[0, n], (n // 8, n // 2 % 4, n % 2, z), is_last,
            )

        @pl.when(is_last)
        def _():
            local = pltpu.make_async_copy(
                fine_p.at[:, pl.ds(248, 8), :], restart.at[pl.ds(2, 4), 15, 1], load_sem.at[0]
            )
            local.start()
            local.wait()

    def fine_beside():
        for n in range(31, -1, -1):
            for low, to, step, index, cond in (
                (2, 0, 1, 1, is_last & (z < 3)),
                (0, 6, -1, 2, is_last & (z > 0)),
            ):
                send(
                    fine_p.at[pl.ds(low, 2), pl.ds(8 * n, 8), :],
                    restart.at[pl.ds(to, 2), n // 2, n % 2], fine_sem.at[index, n],
                    (n // 8, n // 2 % 4, n % 2, turned(z + step)), cond,
                )

    fine_parts = (
        (0, 2, 4, jnp.logical_not(is_last), None), (1, 0, 2, z > 0, z > 0), (2, 6, 2, z < 3, z < 3)
    )

    def fine_direct(index):
        _, low, count, ready_cond, cond = fine_parts[index]
        view = restart.at[pl.ds(low, count), chip, c]
        arrived(view, fine_sem.at[index, mine], ready_cond)
        for dy, dx in plane:
            to = (turned(y + dy), turned(x + dx), c, z)
            send(view, view, fine_sem.at[index, mine], to, cond)

    def fine_across():
        for index, low, count, _, cond in fine_parts:
            for dy, dx in plane:
                other = turned(y + dy) * 4 + turned(x + dx)
                view = restart.at[pl.ds(low, count), other, c]
                arrived(view, fine_sem.at[index, other * 2 + c], cond)
            view = restart.at[pl.ds(low, count), :, c]
            send(view, view, restart_sem.at[index], partner, cond)

    def fine_ready():
        for index, low, count, _, cond in fine_parts:
            arrived(restart.at[pl.ds(low, count), :, 1 - c], restart_sem.at[index], cond)

    fine_own()
    load_r.wait()
    restrict(fine_r, 1, 0.0625)
    for d in (1, 3, 2):
        to = turned(z + d)
        send(
            own.at[1, :, pl.ds(32 * to + 16 * c, 48), :], rate_c.at[layers], rate_sem,
            (y, x, c, to),
        )
    rate_c[layers] = own[1, :, pl.ds(32 * z + 16 * c, 48), :]
    arrived(layer, seed_sem.at[0], in_line & (along != 3))
    for d in (2, 1, -1):
        send(layer, layer, seed_sem.at[0], second(d), in_line)

    def spread_seed():
        arrived(layer, seed_sem.at[0], jnp.logical_not(in_line))
        target = 2 * z + 1 - c
        for d in (1, 3, 2, 0):
            for core in (0, 1):
                to = turned(z + d)
                view = layer.at[pl.ds(32 * to + 16 * core, 48), :]
                cond = None if d else (c != core)
                send(view, seed.at[target], seed_sem.at[1], (y, x, core, to), cond)
        seed[target] = layer[pl.ds(32 * z + 16 * c, 48), :]

    def chunk(da, db):
        return buf.at[slot(da, db)], slot_sem.at[slot(da, db)]

    def across_chip(da, db, cond=None):
        view = buf.at[slot(da, db), :, pl.ds(16 * (1 - c), 48), :]
        send(view, view, slot_sem.at[slot(da, db)], partner, cond)

    def onward(da, db):
        full, sem = chunk(da, db)
        for step in (1, -1):
            send(full, full, sem, second(step))
        across_chip(da, db)

    def relay(da, db, device, h):
        full, sem = chunk(da, db)
        arrived(full, sem)
        view = buf.at[slot(da, db), pl.ds(4 * h, 4)]
        send(view, view, sem, device)

    def near(relay, onward):
        relay(-1, 0, first(1), 0)
        onward(-1, 0)
        relay(1, 0, first(-1), 1)
        onward(1, 0)

    def ring(relay, a):
        for step, h in ((-1, 0), (1, 1)):
            relay(a, step, second(-step), h)
            across_chip(a, step)

    full, sem = chunk(0, 0)
    arrived(full.at[pl.ds(0, 6)], sem)
    for step in (1, -1):
        send(full, full, sem, first(step))
    onward(0, 0)
    near(relay, onward)
    spread_seed()
    other_halos()
    ring(relay, 0)
    arrived(*chunk(2, 0))
    onward(2, 0)
    ring(relay, -1)
    ring(relay, 1)
    arrived(*chunk(0, 2))
    across_chip(0, 2)
    ring(relay, 2)

    def ready(block):
        for a in (-1, 1, 2):
            here = slot(a, 2)
            cond = here // 8 == block
            arrived(*chunk(a, 2), cond)
            across_chip(a, 2, cond)
        for b in range(4):
            other = (block * 4 + b) * 2 + 1 - c
            arrived(buf.at[other, :, rows, :], slot_sem.at[other])

    arrived(rate_c.at[pl.ds(0, 6)], rate_sem)
    arrived(seed.at[pl.ds(0, 7)], seed_sem.at[1])

    state_a[...] = jnp.zeros_like(state_a)
    state_b[...] = jnp.zeros_like(state_b)
    state_a[pl.ds(1, 8), pl.ds(8, 48), :] = seed[...]
    inner = pl.ds(24, 16)
    up = (y, x, 1 - c, turned(z + c))
    down = (y, x, 1 - c, turned(z - 1 + c))

    def run(block, low, count, tiles):
        def body(i, carry):
            t = block * 8 + low + i

            @pl.when(t == 2 * chip)
            def _():
                found[0] = state_a[pl.ds(1, 8), inner, :]

            def at(n, j):
                r = 8 * tiles[j]
                return rate_c[n, pl.ds(r, 8), :], buf[t, n, pl.ds(16 * c + r, 8), :]

            planes = [(k, k, k - 1) for k in range(1, 9)]
            starts = [8 + 8 * tile for tile in tiles]
            coarse_stage(state_a, state_b, planes, starts, at)
            coarse_stage(state_b, state_a, planes, starts, at)
            return carry

        lax.fori_loop(0, count, body, 0)

    for block in range(4):
        active = y >= block
        if block:
            e = block - 1

            def fill(e=e):
                edge_out[e] = state_a[pl.ds(1, 8), inner, :]

            pl.when(active)(fill)
            send(edge_out.at[e], edge_in.at[e, 0], edge_sem.at[e, 0], up, active)
            send(edge_out.at[e], edge_in.at[e, 1], edge_sem.at[e, 1], down, active)
            if block == 1:
                rate_fine()
                fine_beside()
                fine_direct(0)
            if block == 2:
                rate_coarse()
                fine_direct(1)
            if block == 3:
                fine_direct(2)
            arrived(edge_in.at[e, 0], edge_sem.at[e, 0], active)
            arrived(edge_in.at[e, 1], edge_sem.at[e, 1], active)

            def spill(e=e):
                state_a[pl.ds(1, 8), pl.ds(8, 16), :] = edge_in[e, 0]
                state_a[pl.ds(1, 8), pl.ds(40, 16), :] = edge_in[e, 1]

            pl.when(active)(spill)
        ready(block)
        count = jnp.where(y > block, 8, jnp.where(active, 2 * x + 1, 0))
        run(block, 0, jnp.minimum(count, 4), range(6))
        run(block, 4, jnp.maximum(count - 4, 0), range(1, 5))

    found[1] = state_a[pl.ds(1, 8), inner, :]
    here = pl.ds(8 + 16 * slab, 16)
    for d in (1, 3, 2, 0):
        to = turned(z + d)
        end = (to == 0) | (to == 3)
        for core in (0, 1):
            for count, low, cond in (
                (5, jnp.where(to == 0, 0, 3), end),
                (7, jnp.where(to == 1, 0, 1), jnp.logical_not(end)),
            ):
                send(
                    found.at[core, pl.ds(low, count)], start.at[pl.ds(3 + low, count), here, :],
                    state_sem, (y, x, core, to), cond if d else cond & (c != core),
                )
    rate_across()
    zero = jnp.zeros((3, 144, 128), F32)
    start[pl.ds(0, 3)] = zero
    start[pl.ds(11, 3)] = zero
    start[pl.ds(3, 8), here, :] = found[c]

    for index in (0, 1):
        arrived((prev_lo, prev_hi)[index], halo_sem.at[index], (z < 3) if index else (z > 0))
    sides = [
        pltpu.make_async_copy(view, fine_r.at[pl.ds(2 * n, 2)], load_sem.at[1 + n])
        for n, view in enumerate((prev_lo, prev_hi))
    ]
    for copy in sides:
        copy.start()
    for n in range(2):
        warm[1 + n] = 0.125 * pooled(fine_p[2 * n] + fine_p[2 * n + 1], pair, half)
    for copy in sides:
        copy.wait()
    for n in range(2):
        warm[3 * n] = 0.125 * pooled(fine_r[2 * n] + fine_r[2 * n + 1], pair, half)
    for f in range(2):
        near_c[f, pl.ds(2, 2)] = own[f, :, pl.ds(16, 128), :]
    for n, cond in ((0, z > 0), (1, z < 3)):
        arrived(near_c.at[0, pl.ds(4 * n, 2)], near_sem.at[0, n], cond)
        arrived(rate_c_others[n], rate_half_sem.at[2, n], cond)
    fine_across()
    for count, cond in ((5, (z == 0) | (z == 3)), (7, (z == 1) | (z == 2))):
        arrived(start.at[pl.ds(0, count), pl.ds(0, 112), :], state_sem, cond)

    first_low = 2 * z + 1

    def wrapped(ref, low, count):
        for k in range(count):
            ref[low + k, pl.ds(0, 8), :] = ref[low + k, pl.ds(128, 8), :]
            ref[low + k, pl.ds(136, 8), :] = ref[low + k, pl.ds(8, 8), :]

    wrapped(start, 2 * z, 8)

    def rows_of(i):
        def at(n, j):
            r = pl.ds(16 * i + 8 * j, 8)
            return near_c[1, n, r, :], near_c[0, n, r, :]

        return [8 + 16 * i, 16 + 16 * i], at

    def half_one(i, carry):
        starts, at = rows_of(i)
        planes = [(first_low + n, n, n) for n in range(6)]
        coarse_stage(start, mid, planes, starts, at)
        return carry

    lax.fori_loop(0, 8, half_one, 0, unroll=2)

    @pl.when(z == 0)
    def _():
        mid[pl.ds(0, 2)] = jnp.zeros((2, 144, 128), F32)

    @pl.when(z == 3)
    def _():
        mid[pl.ds(4, 2)] = jnp.zeros((2, 144, 128), F32)

    wrapped(mid, 0, 6)

    def half_two(i, carry):
        starts, at = rows_of(i)
        planes = [(n + 1, n, n + 1) for n in range(4)]
        coarse_stage(mid, end_state, planes, starts, at)
        return carry

    lax.fori_loop(0, 8, half_two, 0, unroll=2)
    states[0] = start[pl.ds(2 * z + 2, 4), pl.ds(8, 128), :]
    states[1] = mid[pl.ds(1, 4), pl.ds(8, 128), :] - warm[...]
    states[2] = end_state[:, pl.ds(8, 128), :] - warm[...]

    fine_ready()
    for n, cond in ((0, z > 0), (1, z < 3)):
        arrived((source_lo, source_hi)[n], halo_sem.at[2 + n], cond)
        arrived(rate_others[n], rate_half_sem.at[1, n], cond)
    assert len(waits) <= N_SEND
    for cond, wait in waits:
        guarded(cond, wait)


def fine_kernel(*refs):
    inputs, result = refs[:11], refs[11]
    half, lifted, mixed, base, extra, last, later = refs[12:19]
    held, load_sem = refs[19:30], refs[30]
    out, store_sem = refs[31], refs[32]
    loads = [
        pltpu.make_async_copy(a, b, load_sem.at[n]) for n, (a, b) in enumerate(zip(inputs, held))
    ]
    for n in (10, 9, 0, 1, 2, 3, 4, 5, 6, 7, 8):
        loads[n].start()
    prev, prev_lo, prev_hi, source, source_lo, source_hi, rate, rate_lo, rate_hi, restart, states = held
    z = lax.axis_index("space")
    w = stencil_weights(1.0)
    pair = pair_table(256, 128)
    spread = (
        lax.broadcasted_iota(jnp.int32, (128, 256), 0)
        == lax.broadcasted_iota(jnp.int32, (128, 256), 1) // 2
    ).astype(F32).astype(jnp.bfloat16)

    def prev_layer(k):
        return prev_lo.at[k] if k < 2 else prev_hi.at[k - 6] if k > 5 else prev.at[k - 2]

    def of(low, middle, high, k):
        return low.at[0] if k < 2 else high.at[0] if k > 5 else middle.at[k - 2]

    def inside(k):
        return (z > 0) if k < 2 else (z < 3) if k > 5 else None

    def masked(k, value):
        cond = inside(k)
        return value if cond is None else jnp.where(cond, value, 0.0)

    loads[10].wait()

    def lift(n, change):
        wide = table_dot(change.reshape(512, 128), spread)
        for k in range(4):
            for h in range(2):
                column = wide[128 * k : 128 * k + 128, 128 * h : 128 * h + 128]
                lifted[n, k, h, pl.ds(0, 128, stride=2), :] = column
                lifted[n, k, h, pl.ds(1, 128, stride=2), :] = column

    lift(1, states[1])
    lift(2, states[2])
    loads[9].wait()
    for k in range(4):
        seed_c = 0.125 * pooled(restart[2 * k] + restart[2 * k + 1], pair, half)
        states[0, k] = states[0, k] - seed_c
    lift(0, states[0])

    def share(v):
        return v * pl.reciprocal(1.0 + v * v)

    def put(ref, k, i, value):
        for h in range(2):
            ref[k, h, pl.ds(8 + 8 * i, 8), :] = value[:, 128 * h : 128 * h + 128]

    def row(ref, k, start):
        return jnp.concatenate([ref[k, h, pl.ds(start, 8), :] for h in range(2)], axis=-1)

    def guesses(i, carry):
        r = pl.ds(8 * i, 8)
        for k in range(8):
            lift = [
                jnp.concatenate([lifted[n, k // 2, h, r, :] for h in range(2)], axis=-1)
                for n in range(3)
            ]
            warm = prev_layer(k)[r, :]
            g = [masked(k, v) for v in (restart[k, r, :] + lift[0], warm + lift[1], warm + lift[2])]
            put(mixed, k, i, weights_one[0] * g[0] + weights_one[1] * g[1] + weights_one[2] * g[2])
            if 1 <= k <= 6:
                s = [share(v) for v in g]
                c = of(rate_lo, rate, rate_hi, k)[r, :]
                q = 0.5 * of(source_lo, source, source_hi, k)[r, :]
                base[k - 1, r, :] = (
                    g[0]
                    + c * (weights_one[0] * s[0] + weights_one[1] * s[1] + weights_one[2] * s[2])
                    + q
                )
                extra[k - 1, r, :] = (
                    weights_two[0] * g[0] + (weights_two[1] - 0.5) * g[1] + weights_two[2] * g[2]
                )
                if 2 <= k <= 5:
                    last[k - 2, r, :] = q + c * (
                        weights_two[0] * s[0]
                        + (weights_two[1] - 0.5) * s[1]
                        + weights_two[2] * s[2]
                    )
        return carry

    def wrap(ref, count):
        for k in range(count):
            for h in range(2):
                ref[k, h, pl.ds(0, 8), :] = ref[k, h, pl.ds(256, 8), :]
                ref[k, h, pl.ds(264, 8), :] = ref[k, h, pl.ds(8, 8), :]

    def linear(ref, k, i, below, here, above):
        r = 8 * i + 8
        value = w[0] * here + w[1] * above + w[2] * below
        value += w[3] * row(ref, k, r + 1) + w[4] * row(ref, k, r - 1)
        return value + w[5] * pltpu.roll(here, 255, 1) + w[6] * pltpu.roll(here, 1, 1)

    for n in range(9):
        loads[n].wait()
    lax.fori_loop(0, 32, guesses, 0, unroll=2)
    wrap(mixed, 8)

    def node_one(i, carry):
        r = pl.ds(8 * i, 8)
        planes = [row(mixed, k, 8 + 8 * i) for k in range(8)]
        for k in range(6):
            value = base[k, r, :] + linear(mixed, k + 1, i, *planes[k : k + 3])
            value = masked(0, value) if k == 0 else masked(7, value) if k == 5 else value
            if 1 <= k <= 4:
                out[0, 0, k - 1, r, :] = value
            put(later, k, i, 0.5 * value + extra[k, r, :])
        return carry

    lax.fori_loop(0, 32, node_one, 0, unroll=4)
    wrap(later, 6)
    stores = [
        pltpu.make_async_copy(out.at[0, n], result.at[0, n], store_sem.at[n]) for n in range(2)
    ]
    stores[0].start()

    def node_two(i, carry):
        r = pl.ds(8 * i, 8)
        planes = [row(later, k, 8 + 8 * i) for k in range(6)]
        for k in range(4):
            one = out[0, 0, k, r, :]
            value = one + 0.5 * rate[k, r, :] * share(one) + last[k, r, :]
            out[0, 1, k, r, :] = value + linear(later, k + 1, i, *planes[k : k + 3])
        return carry

    lax.fori_loop(0, 32, node_two, 0, unroll=4)
    stores[1].start()
    for copy in stores:
        copy.wait()


def shards(previous_end, source, rate):
    prev = previous_end[0]
    own = source[0]
    any_space = pl.BlockSpec(memory_space=pl.ANY)
    vmem = pl.BlockSpec(memory_space=pltpu.VMEM)
    dma = pltpu.SemaphoreType.DMA

    def shape(*dims):
        return jax.ShapeDtypeStruct(dims, F32)

    def scratch(*dims):
        return pltpu.VMEM(dims, F32)

    states, restart, *halos = pl.pallas_call(
        chain_kernel,
        out_shape=[shape(3, 4, 128, 128), shape(8, 16, 2, 8, 256)]
        + [shape(2, 256, 256)] * 2
        + [shape(1, 256, 256)] * 4,
        in_specs=[any_space] * 3,
        out_specs=[vmem] + [any_space] * 7,
        scratch_shapes=[
            scratch(4, 256, 256), scratch(4, 256, 256), scratch(4, 256, 256), scratch(256, 128),
            scratch(3, 2, 160, 128), scratch(32, 8, 64, 128), scratch(8, 48, 128),
            scratch(8, 48, 128), scratch(10, 64, 128), scratch(10, 64, 128),
            scratch(3, 8, 16, 128), scratch(3, 2, 8, 16, 128), scratch(2, 8, 16, 128),
            scratch(160, 128), scratch(14, 144, 128), scratch(6, 144, 128), scratch(4, 144, 128),
            scratch(2, 6, 128, 128), scratch(4, 128, 128),
            dma((3,)), dma((N_SEND,)), dma((32,)), dma((3, 32)), dma((2,)), dma, dma((3, 2)), dma,
            dma((4,)), dma((3,)), dma((2, 2)), dma((3, 2)),
        ],
        compiler_params=pltpu.CompilerParams(
            collective_id=0, has_side_effects=True, vmem_limit_bytes=63 * 1024 * 1024
        ),
    )(prev, own, rate)
    prev_lo, prev_hi, source_lo, source_hi, rate_lo, rate_hi = halos
    restart = restart.reshape(8, 256, 256)
    return pl.pallas_call(
        fine_kernel,
        out_shape=shape(1, 2, 4, 256, 256),
        in_specs=[any_space] * 11,
        out_specs=any_space,
        scratch_shapes=[
            scratch(256, 128), scratch(3, 4, 2, 256, 128), scratch(8, 2, 272, 128),
            scratch(6, 256, 256), scratch(6, 256, 256), scratch(4, 256, 256),
            scratch(6, 2, 272, 128),
            scratch(4, 256, 256), scratch(2, 256, 256), scratch(2, 256, 256),
            scratch(4, 256, 256), scratch(1, 256, 256), scratch(1, 256, 256),
            scratch(4, 256, 256), scratch(1, 256, 256), scratch(1, 256, 256),
            scratch(8, 256, 256), scratch(3, 4, 128, 128), dma((11,)),
            scratch(1, 2, 4, 256, 256), dma((2,)),
        ],
        compiler_params=pltpu.CompilerParams(vmem_limit_bytes=63 * 1024 * 1024),
    )(prev, prev_lo, prev_hi, own, source_lo, source_hi, rate, rate_lo, rate_hi, restart, states)


def solution(mesh):
    torus = Mesh(
        mesh.devices.reshape(4, 4, 2, mesh.shape["space"]), ("tm_0", "tm_1", "tm_2", "space")
    )
    placed = (P(TM, "space", None, None), P(TM, "space", None, None), P("space", None, None))
    return jax.shard_map(
        shards,
        mesh=torus,
        in_specs=placed,
        out_specs=P(TM, None, "space", None, None),
        check_vma=False,
    )
```

```python
import jax
import jax.numpy as jnp
from jax import lax
from jax.experimental import pallas as pl
from jax.experimental.pallas import tpu as pltpu
from jax.sharding import Mesh
from jax.sharding import PartitionSpec as P

TM = ("tm_0", "tm_1", "tm_2")
AXES = TM + ("space",)
MESH = pl.DeviceIdType.MESH
F32 = jnp.float32

diffusion = 0.1
speed_z = 0.4
speed_x = 0.3
speed_y = 0.2
weights_one = (5.0 / 24.0, 1.0 / 3.0, -1.0 / 24.0)
weights_two = (-1.0 / 24.0, 1.0 / 3.0, 5.0 / 24.0)


def stencil_weights(spacing):
    d = diffusion / (spacing * spacing)
    out = [-6.0 * d]
    for speed in (speed_z, speed_x, speed_y):
        out += [d - speed / (2.0 * spacing), d + speed / (2.0 * spacing)]
    return out


def pair_table(fine, coarse):
    rows = lax.broadcasted_iota(jnp.int32, (fine, coarse), 0) // 2
    columns = lax.broadcasted_iota(jnp.int32, (fine, coarse), 1)
    return (rows == columns).astype(F32).astype(jnp.bfloat16)


def table_dot(value, table):
    out = None
    for _ in range(3):
        part = value.astype(jnp.bfloat16)
        value = value - part.astype(F32)
        term = jnp.dot(part, table, preferred_element_type=F32)
        out = term if out is None else out + term
    return out


def pooled(total, pair, scratch):
    scratch[...] = table_dot(total, pair)
    return scratch[pl.ds(0, 128, stride=2), :] + scratch[pl.ds(1, 128, stride=2), :]


def coarse_stage(src, dst, planes, starts, at):
    w = [0.5 * v for v in stencil_weights(2.0)]
    for j, r in enumerate(starts):
        below = src[planes[0][0] - 1, pl.ds(r, 8), :]
        here = src[planes[0][0], pl.ds(r, 8), :]
        for k, to, n in planes:
            above = src[k + 1, pl.ds(r, 8), :]
            rate, source = at(n, j)
            out = (1.0 + w[0]) * here + source
            out += w[1] * above + w[2] * below
            out += w[3] * src[k, pl.ds(r + 1, 8), :] + w[4] * src[k, pl.ds(r - 1, 8), :]
            out += w[5] * pltpu.roll(here, 127, 1) + w[6] * pltpu.roll(here, 1, 1)
            out += rate * here * pl.reciprocal(1.0 + here * here)
            dst[to, pl.ds(r, 8), :] = out
            below, here = here, above


N_SEND = 320


def chain_kernel(
    prev, source, rate,
    states, restart, prev_lo, prev_hi, source_lo, source_hi, rate_lo, rate_hi,
    fine_s, fine_r, fine_p, half, own, buf, rate_c, seed, state_a, state_b,
    edge_out, edge_in, found, layer, start, mid, end_state, near_c, warm,
    load_sem, send_sem, slot_sem, fine_sem, seed_sem, rate_sem, edge_sem, state_sem, halo_sem,
    restart_sem, near_sem, rate_half_sem,
):
    y, x, c, z = (lax.axis_index(name) for name in AXES)
    chip = y * 4 + x
    mine = chip * 2 + c
    slab = 2 * z + c
    is_last = mine == 31
    partner = (y, x, 1 - c, z)
    waits = []

    def guarded(cond, action):
        if cond is None:
            action()
        else:
            pl.when(cond)(action)

    def send(src, dst, sem, device, cond=None):
        index = len(waits)

        def build():
            return pltpu.make_async_remote_copy(
                src_ref=src, dst_ref=dst, send_sem=send_sem.at[index], recv_sem=sem,
                device_id=device, device_id_type=MESH,
            )

        waits.append((cond, lambda: build().wait_send()))
        guarded(cond, lambda: build().start())

    def arrived(view, sem, cond=None):
        def wait():
            pltpu.make_async_remote_copy(
                src_ref=view, dst_ref=view, send_sem=send_sem.at[0], recv_sem=sem,
                device_id=partner, device_id_type=MESH,
            ).wait_recv()

        guarded(cond, wait)

    def turned(value):
        return lax.rem(value + 8, 4)

    def first(step):
        return (turned(y + step * c), turned(x + step * (1 - c)), c, z)

    def second(step):
        return (turned(y + step * (1 - c)), turned(x + step * c), c, z)

    def slot(da, db):
        return (turned(y + da * c + db * (1 - c)) * 4 + turned(x + da * (1 - c) + db * c)) * 2 + c

    load_p = pltpu.make_async_copy(prev, fine_p, load_sem.at[0])
    load_s = pltpu.make_async_copy(source, fine_s, load_sem.at[1])
    load_r = pltpu.make_async_copy(rate, fine_r, load_sem.at[2])
    load_p.start()
    load_s.start()
    load_r.start()
    barrier = pltpu.get_barrier_semaphore()
    plane = [(dy, dx) for dy in range(4) for dx in range(4) if dy or dx]
    peers = [(turned(y + dy), turned(x + dx), c, z) for dy, dx in plane]
    peers += [(y, x, c, turned(z + d)) for d in (1, 2, 3)]
    peers += [(y, x, 1 - c, turned(z + d)) for d in (0, 1, 2, 3)]
    for device in peers:
        pl.semaphore_signal(barrier, inc=1, device_id=device, device_id_type=MESH)

    def greet(step):
        to = (3, 3, 1, turned(z + step))
        pl.semaphore_signal(barrier, inc=1, device_id=to, device_id_type=MESH)

    pl.when(jnp.logical_not(is_last))(lambda: greet(0))
    pl.when(z > 0)(lambda: greet(-1))
    pl.when(z < 3)(lambda: greet(1))
    inner_z = (z > 0) & (z < 3)
    more = jnp.where(is_last, jnp.where(inner_z, 95, 63), 0)

    pair = pair_table(256, 128)

    def restrict(fine, index, scale):
        for k in range(2):
            total = scale * pooled(fine[2 * k] + fine[2 * k + 1], pair, half)
            own[index, k, pl.ds(16, 128), :] = total
            own[index, k, pl.ds(0, 16), :] = total[112:128]
            own[index, k, pl.ds(144, 16), :] = total[0:16]

    load_p.wait()
    pl.when(is_last)(lambda: restrict(fine_p, 2, 0.125))
    load_s.wait()
    restrict(fine_s, 0, 0.0625)
    pl.semaphore_wait(barrier, len(peers) + more)

    layers = pl.ds(2 * z, 2)
    rows = pl.ds(16 * c, 48)
    along = x * (1 - c) + y * c
    across = y * (1 - c) + x * c
    in_line = across == 3
    is_root = in_line & (along == 3)

    send(own.at[2, 1], layer, seed_sem.at[0], partner, is_last)

    def seed_self():
        layer[...] = own[2, 0]

    pl.when(is_last)(seed_self)

    for d in (1, 3, 2):
        to = turned(z + d)
        send(
            own.at[0, :, pl.ds(32 * to, 64), :], buf.at[mine, layers], slot_sem.at[mine],
            (y, x, c, to),
        )
    buf[mine, layers] = own[0, :, pl.ds(32 * z, 64), :]
    arrived(layer, seed_sem.at[0], mine == 30)
    for d in (2, 1, -1):
        send(layer, layer, seed_sem.at[0], first(d), is_root)

    def fine_halo(field, low, high, width, index):
        send(
            field.at[pl.ds(4 - width, width)], low, halo_sem.at[index], (y, x, c, turned(z + 1)),
            z < 3,
        )
        send(
            field.at[pl.ds(0, width)], high, halo_sem.at[index + 1], (y, x, c, turned(z - 1)),
            z > 0,
        )

    def along_z(pieces, sems, index):
        for (src, dst), n, step, cond in zip(pieces, (0, 1), (1, -1), (z < 3, z > 0)):
            send(src, dst, sems.at[index, n], (y, x, c, turned(z + step)), cond)

    def other_halos():
        src = own.at[0, :, pl.ds(16, 128), :]
        along_z([(src, near_c.at[0, pl.ds(4 * n, 2)]) for n in range(2)], near_sem, 0)
        fine_halo(source, source_lo, source_hi, 1, 2)

    rate_rows = pl.ds(128 * c, 128)
    rate_views = [view.at[:, rate_rows, :] for view in (rate_lo, rate_hi)]
    rate_c_views = [near_c.at[1, pl.ds(4 * n + c, 1)] for n in range(2)]
    rate_others = [view.at[:, pl.ds(128 * (1 - c), 128), :] for view in (rate_lo, rate_hi)]
    rate_c_others = [near_c.at[1, pl.ds(4 * n + 1 - c, 1)] for n in range(2)]

    def rate_fine():
        srcs = [rate.at[pl.ds(3 * (1 - n), 1), rate_rows, :] for n in range(2)]
        along_z(zip(srcs, rate_views), rate_half_sem, 0)

    def rate_coarse():
        src = own.at[1, pl.ds(c, 1), pl.ds(16, 128), :]
        along_z([(src, view) for view in rate_c_views], near_sem, 1)

    def rate_across():
        for views, sems, index in ((rate_c_views, near_sem, 1), (rate_views, rate_half_sem, 0)):
            for n, cond in ((0, z > 0), (1, z < 3)):
                arrived(views[n], sems.at[index, n], cond)
                send(views[n], views[n], rate_half_sem.at[1 + index, n], partner, cond)

    fine_halo(prev, prev_lo, prev_hi, 2, 0)

    def fine_own():
        for n in range(30, -1, -1):
            send(
                fine_p.at[:, pl.ds(8 * n, 8), :], restart.at[pl.ds(2, 4), n // 2, n % 2],
                fine_sem.at[0, n], (n // 8, n // 2 % 4, n % 2, z), is_last,
            )

        @pl.when(is_last)
        def _():
            local = pltpu.make_async_copy(
                fine_p.at[:, pl.ds(248, 8), :], restart.at[pl.ds(2, 4), 15, 1], load_sem.at[0]
            )
            local.start()
            local.wait()

    def fine_beside():
        for n in range(31, -1, -1):
            for low, to, step, index, cond in (
                (2, 0, 1, 1, is_last & (z < 3)),
                (0, 6, -1, 2, is_last & (z > 0)),
            ):
                send(
                    fine_p.at[pl.ds(low, 2), pl.ds(8 * n, 8), :],
                    restart.at[pl.ds(to, 2), n // 2, n % 2], fine_sem.at[index, n],
                    (n // 8, n // 2 % 4, n % 2, turned(z + step)), cond,
                )

    fine_parts = (
        (0, 2, 4, jnp.logical_not(is_last), None), (1, 0, 2, z > 0, z > 0), (2, 6, 2, z < 3, z < 3)
    )

    def fine_direct(index):
        _, low, count, ready_cond, cond = fine_parts[index]
        view = restart.at[pl.ds(low, count), chip, c]
        arrived(view, fine_sem.at[index, mine], ready_cond)
        for dy, dx in plane:
            to = (turned(y + dy), turned(x + dx), c, z)
            send(view, view, fine_sem.at[index, mine], to, cond)

    def fine_across():
        for index, low, count, _, cond in fine_parts:
            for dy, dx in plane:
                other = turned(y + dy) * 4 + turned(x + dx)
                view = restart.at[pl.ds(low, count), other, c]
                arrived(view, fine_sem.at[index, other * 2 + c], cond)
            view = restart.at[pl.ds(low, count), :, c]
            send(view, view, restart_sem.at[index], partner, cond)

    def fine_ready():
        for index, low, count, _, cond in fine_parts:
            arrived(restart.at[pl.ds(low, count), :, 1 - c], restart_sem.at[index], cond)

    fine_own()
    load_r.wait()
    restrict(fine_r, 1, 0.0625)
    for d in (1, 3, 2):
        to = turned(z + d)
        send(
            own.at[1, :, pl.ds(32 * to + 16 * c, 48), :], rate_c.at[layers], rate_sem,
            (y, x, c, to),
        )
    rate_c[layers] = own[1, :, pl.ds(32 * z + 16 * c, 48), :]
    arrived(layer, seed_sem.at[0], in_line & (along != 3))
    for d in (2, 1, -1):
        send(layer, layer, seed_sem.at[0], second(d), in_line)

    def spread_seed():
        arrived(layer, seed_sem.at[0], jnp.logical_not(in_line))
        target = 2 * z + 1 - c
        for d in (1, 3, 2, 0):
            for core in (0, 1):
                to = turned(z + d)
                view = layer.at[pl.ds(32 * to + 16 * core, 48), :]
                cond = None if d else (c != core)
                send(view, seed.at[target], seed_sem.at[1], (y, x, core, to), cond)
        seed[target] = layer[pl.ds(32 * z + 16 * c, 48), :]

    def chunk(da, db):
        return buf.at[slot(da, db)], slot_sem.at[slot(da, db)]

    def across_chip(da, db, cond=None):
        view = buf.at[slot(da, db), :, pl.ds(16 * (1 - c), 48), :]
        send(view, view, slot_sem.at[slot(da, db)], partner, cond)

    def onward(da, db):
        full, sem = chunk(da, db)
        for step in (1, -1):
            send(full, full, sem, second(step))
        across_chip(da, db)

    def relay(da, db, device, h):
        full, sem = chunk(da, db)
        arrived(full, sem)
        view = buf.at[slot(da, db), pl.ds(4 * h, 4)]
        send(view, view, sem, device)

    def near(relay, onward):
        relay(-1, 0, first(1), 0)
        onward(-1, 0)
        relay(1, 0, first(-1), 1)
        onward(1, 0)

    def ring(relay, a):
        for step, h in ((-1, 0), (1, 1)):
            relay(a, step, second(-step), h)
            across_chip(a, step)

    full, sem = chunk(0, 0)
    arrived(full.at[pl.ds(0, 6)], sem)
    for step in (1, -1):
        send(full, full, sem, first(step))
    onward(0, 0)
    near(relay, onward)
    spread_seed()
    other_halos()
    ring(relay, 0)
    arrived(*chunk(2, 0))
    onward(2, 0)
    ring(relay, -1)
    ring(relay, 1)
    arrived(*chunk(0, 2))
    across_chip(0, 2)
    ring(relay, 2)

    def ready(block):
        for a in (-1, 1, 2):
            here = slot(a, 2)
            cond = here // 8 == block
            arrived(*chunk(a, 2), cond)
            across_chip(a, 2, cond)
        for b in range(4):
            other = (block * 4 + b) * 2 + 1 - c
            arrived(buf.at[other, :, rows, :], slot_sem.at[other])

    arrived(rate_c.at[pl.ds(0, 6)], rate_sem)
    arrived(seed.at[pl.ds(0, 7)], seed_sem.at[1])

    state_a[...] = jnp.zeros_like(state_a)
    state_b[...] = jnp.zeros_like(state_b)
    state_a[pl.ds(1, 8), pl.ds(8, 48), :] = seed[...]
    inner = pl.ds(24, 16)
    up = (y, x, 1 - c, turned(z + c))
    down = (y, x, 1 - c, turned(z - 1 + c))

    def run(block, low, count, tiles):
        def body(i, carry):
            t = block * 8 + low + i

            @pl.when(t == 2 * chip)
            def _():
                found[0] = state_a[pl.ds(1, 8), inner, :]

            def at(n, j):
                r = 8 * tiles[j]
                return rate_c[n, pl.ds(r, 8), :], buf[t, n, pl.ds(16 * c + r, 8), :]

            planes = [(k, k, k - 1) for k in range(1, 9)]
            starts = [8 + 8 * tile for tile in tiles]
            coarse_stage(state_a, state_b, planes, starts, at)
            coarse_stage(state_b, state_a, planes, starts, at)
            return carry

        lax.fori_loop(0, count, body, 0)

    for block in range(4):
        active = y >= block
        if block:
            e = block - 1

            def fill(e=e):
                edge_out[e] = state_a[pl.ds(1, 8), inner, :]

            pl.when(active)(fill)
            send(edge_out.at[e], edge_in.at[e, 0], edge_sem.at[e, 0], up, active)
            send(edge_out.at[e], edge_in.at[e, 1], edge_sem.at[e, 1], down, active)
            if block == 1:
                rate_fine()
                fine_beside()
                fine_direct(0)
            if block == 2:
                rate_coarse()
                fine_direct(1)
            if block == 3:
                fine_direct(2)
            arrived(edge_in.at[e, 0], edge_sem.at[e, 0], active)
            arrived(edge_in.at[e, 1], edge_sem.at[e, 1], active)

            def spill(e=e):
                state_a[pl.ds(1, 8), pl.ds(8, 16), :] = edge_in[e, 0]
                state_a[pl.ds(1, 8), pl.ds(40, 16), :] = edge_in[e, 1]

            pl.when(active)(spill)
        ready(block)
        count = jnp.where(y > block, 8, jnp.where(active, 2 * x + 1, 0))
        run(block, 0, jnp.minimum(count, 4), range(6))
        run(block, 4, jnp.maximum(count - 4, 0), range(1, 5))

    found[1] = state_a[pl.ds(1, 8), inner, :]
    here = pl.ds(8 + 16 * slab, 16)
    for d in (1, 3, 2, 0):
        to = turned(z + d)
        end = (to == 0) | (to == 3)
        for core in (0, 1):
            for count, low, cond in (
                (5, jnp.where(to == 0, 0, 3), end),
                (7, jnp.where(to == 1, 0, 1), jnp.logical_not(end)),
            ):
                send(
                    found.at[core, pl.ds(low, count)], start.at[pl.ds(3 + low, count), here, :],
                    state_sem, (y, x, core, to), cond if d else cond & (c != core),
                )
    rate_across()
    zero = jnp.zeros((3, 144, 128), F32)
    start[pl.ds(0, 3)] = zero
    start[pl.ds(11, 3)] = zero
    start[pl.ds(3, 8), here, :] = found[c]

    for index in (0, 1):
        arrived((prev_lo, prev_hi)[index], halo_sem.at[index], (z < 3) if index else (z > 0))
    sides = [
        pltpu.make_async_copy(view, fine_r.at[pl.ds(2 * n, 2)], load_sem.at[1 + n])
        for n, view in enumerate((prev_lo, prev_hi))
    ]
    for copy in sides:
        copy.start()
    for n in range(2):
        warm[1 + n] = 0.125 * pooled(fine_p[2 * n] + fine_p[2 * n + 1], pair, half)
    for copy in sides:
        copy.wait()
    for n in range(2):
        warm[3 * n] = 0.125 * pooled(fine_r[2 * n] + fine_r[2 * n + 1], pair, half)
    for f in range(2):
        near_c[f, pl.ds(2, 2)] = own[f, :, pl.ds(16, 128), :]
    for n, cond in ((0, z > 0), (1, z < 3)):
        arrived(near_c.at[0, pl.ds(4 * n, 2)], near_sem.at[0, n], cond)
        arrived(rate_c_others[n], rate_half_sem.at[2, n], cond)
    fine_across()
    for count, cond in ((5, (z == 0) | (z == 3)), (7, (z == 1) | (z == 2))):
        arrived(start.at[pl.ds(0, count), pl.ds(0, 112), :], state_sem, cond)

    first_low = 2 * z + 1

    def wrapped(ref, low, count):
        for k in range(count):
            ref[low + k, pl.ds(0, 8), :] = ref[low + k, pl.ds(128, 8), :]
            ref[low + k, pl.ds(136, 8), :] = ref[low + k, pl.ds(8, 8), :]

    wrapped(start, 2 * z, 8)

    def rows_of(i):
        def at(n, j):
            r = pl.ds(16 * i + 8 * j, 8)
            return near_c[1, n, r, :], near_c[0, n, r, :]

        return [8 + 16 * i, 16 + 16 * i], at

    def half_one(i, carry):
        starts, at = rows_of(i)
        planes = [(first_low + n, n, n) for n in range(6)]
        coarse_stage(start, mid, planes, starts, at)
        return carry

    lax.fori_loop(0, 8, half_one, 0, unroll=2)

    @pl.when(z == 0)
    def _():
        mid[pl.ds(0, 2)] = jnp.zeros((2, 144, 128), F32)

    @pl.when(z == 3)
    def _():
        mid[pl.ds(4, 2)] = jnp.zeros((2, 144, 128), F32)

    wrapped(mid, 0, 6)

    def half_two(i, carry):
        starts, at = rows_of(i)
        planes = [(n + 1, n, n + 1) for n in range(4)]
        coarse_stage(mid, end_state, planes, starts, at)
        return carry

    lax.fori_loop(0, 8, half_two, 0, unroll=2)
    states[0] = start[pl.ds(2 * z + 2, 4), pl.ds(8, 128), :]
    states[1] = mid[pl.ds(1, 4), pl.ds(8, 128), :] - warm[...]
    states[2] = end_state[:, pl.ds(8, 128), :] - warm[...]

    fine_ready()
    for n, cond in ((0, z > 0), (1, z < 3)):
        arrived((source_lo, source_hi)[n], halo_sem.at[2 + n], cond)
        arrived(rate_others[n], rate_half_sem.at[1, n], cond)
    assert len(waits) <= N_SEND
    for cond, wait in waits:
        guarded(cond, wait)


def fine_kernel(*refs):
    inputs, result = refs[:11], refs[11]
    half, lifted, mixed, base, extra, last, later = refs[12:19]
    held, load_sem = refs[19:30], refs[30]
    out, store_sem = refs[31], refs[32]
    loads = [
        pltpu.make_async_copy(a, b, load_sem.at[n]) for n, (a, b) in enumerate(zip(inputs, held))
    ]
    for n in (10, 9, 0, 1, 2, 3, 4, 5, 6, 7, 8):
        loads[n].start()
    prev, prev_lo, prev_hi, source, source_lo, source_hi, rate, rate_lo, rate_hi, restart, states = held
    z = lax.axis_index("space")
    w = stencil_weights(1.0)
    pair = pair_table(256, 128)
    spread = (
        lax.broadcasted_iota(jnp.int32, (128, 256), 0)
        == lax.broadcasted_iota(jnp.int32, (128, 256), 1) // 2
    ).astype(F32).astype(jnp.bfloat16)

    def prev_layer(k):
        return prev_lo.at[k] if k < 2 else prev_hi.at[k - 6] if k > 5 else prev.at[k - 2]

    def of(low, middle, high, k):
        return low.at[0] if k < 2 else high.at[0] if k > 5 else middle.at[k - 2]

    def inside(k):
        return (z > 0) if k < 2 else (z < 3) if k > 5 else None

    def masked(k, value):
        cond = inside(k)
        return value if cond is None else jnp.where(cond, value, 0.0)

    loads[10].wait()

    def lift(n, change):
        wide = table_dot(change.reshape(512, 128), spread)
        for k in range(4):
            for h in range(2):
                column = wide[128 * k : 128 * k + 128, 128 * h : 128 * h + 128]
                lifted[n, k, h, pl.ds(0, 128, stride=2), :] = column
                lifted[n, k, h, pl.ds(1, 128, stride=2), :] = column

    lift(1, states[1])
    lift(2, states[2])
    loads[9].wait()
    for k in range(4):
        seed_c = 0.125 * pooled(restart[2 * k] + restart[2 * k + 1], pair, half)
        states[0, k] = states[0, k] - seed_c
    lift(0, states[0])

    def share(v):
        return v * pl.reciprocal(1.0 + v * v)

    def put(ref, k, i, value):
        for h in range(2):
            ref[k, h, pl.ds(8 + 8 * i, 8), :] = value[:, 128 * h : 128 * h + 128]

    def row(ref, k, start):
        return jnp.concatenate([ref[k, h, pl.ds(start, 8), :] for h in range(2)], axis=-1)

    def guesses(i, carry):
        r = pl.ds(8 * i, 8)
        for k in range(8):
            lift = [
                jnp.concatenate([lifted[n, k // 2, h, r, :] for h in range(2)], axis=-1)
                for n in range(3)
            ]
            warm = prev_layer(k)[r, :]
            g = [masked(k, v) for v in (restart[k, r, :] + lift[0], warm + lift[1], warm + lift[2])]
            put(mixed, k, i, weights_one[0] * g[0] + weights_one[1] * g[1] + weights_one[2] * g[2])
            if 1 <= k <= 6:
                s = [share(v) for v in g]
                c = of(rate_lo, rate, rate_hi, k)[r, :]
                q = 0.5 * of(source_lo, source, source_hi, k)[r, :]
                base[k - 1, r, :] = (
                    g[0]
                    + c * (weights_one[0] * s[0] + weights_one[1] * s[1] + weights_one[2] * s[2])
                    + q
                )
                extra[k - 1, r, :] = (
                    weights_two[0] * g[0] + (weights_two[1] - 0.5) * g[1] + weights_two[2] * g[2]
                )
                if 2 <= k <= 5:
                    last[k - 2, r, :] = q + c * (
                        weights_two[0] * s[0]
                        + (weights_two[1] - 0.5) * s[1]
                        + weights_two[2] * s[2]
                    )
        return carry

    def wrap(ref, count):
        for k in range(count):
            for h in range(2):
                ref[k, h, pl.ds(0, 8), :] = ref[k, h, pl.ds(256, 8), :]
                ref[k, h, pl.ds(264, 8), :] = ref[k, h, pl.ds(8, 8), :]

    def linear(ref, k, i, below, here, above):
        r = 8 * i + 8
        value = w[0] * here + w[1] * above + w[2] * below
        value += w[3] * row(ref, k, r + 1) + w[4] * row(ref, k, r - 1)
        return value + w[5] * pltpu.roll(here, 255, 1) + w[6] * pltpu.roll(here, 1, 1)

    for n in range(9):
        loads[n].wait()
    lax.fori_loop(0, 32, guesses, 0, unroll=2)
    wrap(mixed, 8)

    def node_one(i, carry):
        r = pl.ds(8 * i, 8)
        planes = [row(mixed, k, 8 + 8 * i) for k in range(8)]
        for k in range(6):
            value = base[k, r, :] + linear(mixed, k + 1, i, *planes[k : k + 3])
            value = masked(0, value) if k == 0 else masked(7, value) if k == 5 else value
            if 1 <= k <= 4:
                out[0, 0, k - 1, r, :] = value
            put(later, k, i, 0.5 * value + extra[k, r, :])
        return carry

    lax.fori_loop(0, 32, node_one, 0, unroll=8)
    wrap(later, 6)
    stores = [
        pltpu.make_async_copy(out.at[0, n], result.at[0, n], store_sem.at[n]) for n in range(2)
    ]
    stores[0].start()

    def node_two(i, carry):
        r = pl.ds(8 * i, 8)
        planes = [row(later, k, 8 + 8 * i) for k in range(6)]
        for k in range(4):
            one = out[0, 0, k, r, :]
            value = one + 0.5 * rate[k, r, :] * share(one) + last[k, r, :]
            out[0, 1, k, r, :] = value + linear(later, k + 1, i, *planes[k : k + 3])
        return carry

    lax.fori_loop(0, 32, node_two, 0, unroll=8)
    stores[1].start()
    for copy in stores:
        copy.wait()


def shards(previous_end, source, rate):
    prev = previous_end[0]
    own = source[0]
    any_space = pl.BlockSpec(memory_space=pl.ANY)
    vmem = pl.BlockSpec(memory_space=pltpu.VMEM)
    dma = pltpu.SemaphoreType.DMA

    def shape(*dims):
        return jax.ShapeDtypeStruct(dims, F32)

    def scratch(*dims):
        return pltpu.VMEM(dims, F32)

    states, restart, *halos = pl.pallas_call(
        chain_kernel,
        out_shape=[shape(3, 4, 128, 128), shape(8, 16, 2, 8, 256)]
        + [shape(2, 256, 256)] * 2
        + [shape(1, 256, 256)] * 4,
        in_specs=[any_space] * 3,
        out_specs=[vmem] + [any_space] * 7,
        scratch_shapes=[
            scratch(4, 256, 256), scratch(4, 256, 256), scratch(4, 256, 256), scratch(256, 128),
            scratch(3, 2, 160, 128), scratch(32, 8, 64, 128), scratch(8, 48, 128),
            scratch(8, 48, 128), scratch(10, 64, 128), scratch(10, 64, 128),
            scratch(3, 8, 16, 128), scratch(3, 2, 8, 16, 128), scratch(2, 8, 16, 128),
            scratch(160, 128), scratch(14, 144, 128), scratch(6, 144, 128), scratch(4, 144, 128),
            scratch(2, 6, 128, 128), scratch(4, 128, 128),
            dma((3,)), dma((N_SEND,)), dma((32,)), dma((3, 32)), dma((2,)), dma, dma((3, 2)), dma,
            dma((4,)), dma((3,)), dma((2, 2)), dma((3, 2)),
        ],
        compiler_params=pltpu.CompilerParams(
            collective_id=0, has_side_effects=True, vmem_limit_bytes=63 * 1024 * 1024
        ),
    )(prev, own, rate)
    prev_lo, prev_hi, source_lo, source_hi, rate_lo, rate_hi = halos
    restart = restart.reshape(8, 256, 256)
    return pl.pallas_call(
        fine_kernel,
        out_shape=shape(1, 2, 4, 256, 256),
        in_specs=[any_space] * 11,
        out_specs=any_space,
        scratch_shapes=[
            scratch(256, 128), scratch(3, 4, 2, 256, 128), scratch(8, 2, 272, 128),
            scratch(6, 256, 256), scratch(6, 256, 256), scratch(4, 256, 256),
            scratch(6, 2, 272, 128),
            scratch(4, 256, 256), scratch(2, 256, 256), scratch(2, 256, 256),
            scratch(4, 256, 256), scratch(1, 256, 256), scratch(1, 256, 256),
            scratch(4, 256, 256), scratch(1, 256, 256), scratch(1, 256, 256),
            scratch(8, 256, 256), scratch(3, 4, 128, 128), dma((11,)),
            scratch(1, 2, 4, 256, 256), dma((2,)),
        ],
        compiler_params=pltpu.CompilerParams(vmem_limit_bytes=63 * 1024 * 1024),
    )(prev, prev_lo, prev_hi, own, source_lo, source_hi, rate, rate_lo, rate_hi, restart, states)


def solution(mesh):
    torus = Mesh(
        mesh.devices.reshape(4, 4, 2, mesh.shape["space"]), ("tm_0", "tm_1", "tm_2", "space")
    )
    placed = (P(TM, "space", None, None), P(TM, "space", None, None), P("space", None, None))
    return jax.shard_map(
        shards,
        mesh=torus,
        in_specs=placed,
        out_specs=P(TM, None, "space", None, None),
        check_vma=False,
    )
```
